32 devices in a mesh: member: 2 (over core), section: 4 (over y, x), atoms: 4 (over z).
Axes of the slice: x: 2, y: 2, z: 4, core: 2. Of those that a mesh axis runs over, the one named last changes fastest.
Arguments:
- positions: float32 [8, 3, 512], P(None, None, 'atoms'), may hold values from -8 to 8
- atom_types: int32 [8, 512], P(None, 'atoms'), may hold values from 0 to 127
- neighbors: int32 [8, 512, 128], P(None, 'atoms'), may hold values from 0 to 511
- nbr_mask: int32 [8, 512, 128], P(None, 'atoms'), may hold values 0 or 1
- type_table: bfloat16 [2, 128, 128], P('member'), may hold values from -6 to 6
- norm_gain: bfloat16 [2, 4, 128], P('member', 'section'), may hold values from 0.25 to 1.75
- proj_weight: bfloat16 [2, 4, 128, 384], P('member', 'section'), may hold values from -0.5 to 0.5
- out_weight: bfloat16 [2, 4, 128, 128], P('member', 'section'), may hold values from -0.5 to 0.5
- force_coef: bfloat16 [2, 4, 4], P('member', 'section'), may hold values from -48 to 48
Outputs:
- atom_dev: float32 [8, 512], P('section', 'atoms')
- max_dev: float32 [8], P('section')
- mean_force: float32 [8, 3, 512], P('section', None, 'atoms')
The draws below stay inside these ranges and needn't reach their ends.
Inputs may be any that keep to these rules, and one draw needn't show every extreme that they name: `neighbors`: indices of atoms of the same frame, repeats and the atom itself allowed.
All inputs are finite; a program needn't handle non-finite values. No bound on the sum of `nbr_mask` on one device may be relied on, other than what follows from the above.
Results may differ from the reference program's by a relative error of at most 0.013.
Values may be sent and summed in bfloat16 or wider, within the bound.
No kernel may reach another device: no remote copies, remote signals or barrier semaphores. Data moves between devices by JAX's collectives and lax.ppermute only.
A program may use at most 64 MiB of HBM per device.

```python
import math
import jax
import jax.numpy as jnp
from jax import lax

D = 128
HEADS = 4
NBR = 128
NTYPES = 128
MICRO = 8
HEAD_DIM = 32
ATOMS = 512
MEMBERS = 2
SECTIONS = 4


def with_ends(array, stream_key, least, largest):
    index_at = [jax.random.randint(jax.random.fold_in(stream_key, axis), (), 0, length) for axis, length in enumerate(array.shape)]
    widest = array.shape.index(max(array.shape))
    next_to = index_at[:widest] + [(index_at[widest] + 1) % array.shape[widest]] + index_at[widest + 1:]
    return array.at[tuple(index_at)].set(least).at[tuple(next_to)].set(largest)


def block_scale(own_key, shape, pieces, smallest, top_value):
    def one(position, parts):
        draws = jax.random.uniform(jax.random.fold_in(jax.random.fold_in(own_key, 6), position), (parts,), jnp.float32, smallest / len(pieces), top_value / len(pieces))
        return jnp.repeat(jnp.exp(draws), shape[position] // parts).reshape((-1,) + (1,) * (len(shape) - position - 1))

    loudness = one(*pieces[0])
    for cut in pieces[1:]:
        loudness = loudness * one(*cut)
    return loudness


def gaussian(stream_key, extent, deviation, bound, cuts=(), kind=jnp.bfloat16):
    level = block_scale(stream_key, extent, cuts, -0.22, 0.18) if cuts else 1.0
    result = jax.random.normal(stream_key, extent, jnp.float32) * deviation * level
    return jnp.minimum(jnp.maximum(result, -bound), bound).astype(kind)


def setup_inputs(seed: int = 0) -> dict:
    streams_of = jax.random.split(jax.random.key(seed), 10)
    return {
        "positions": gaussian(streams_of[0], (MICRO, 3, ATOMS), 2.0, 8.0, ((2, 4),), jnp.float32),
        "atom_types": with_ends(jax.random.randint(streams_of[1], (MICRO, ATOMS), 0, NTYPES), jax.random.fold_in(streams_of[1], 1), 0, NTYPES - 1).astype(jnp.int32),
        "neighbors": with_ends(jax.random.randint(streams_of[2], (MICRO, ATOMS, NBR), 0, ATOMS), jax.random.fold_in(streams_of[2], 1), 0, ATOMS - 1).astype(jnp.int32),
        "nbr_mask": with_ends((jax.random.randint(streams_of[3], (MICRO, ATOMS, NBR), 0, 4) < 3).astype(jnp.int32), jax.random.fold_in(streams_of[3], 1), 0, 1),
        "type_table": gaussian(streams_of[4], (MEMBERS, NTYPES, D), 1.0, 6.0, ((0, 2),)),
        "norm_gain": jnp.clip(1.0 + 0.15 * jax.random.normal(streams_of[5], (MEMBERS, SECTIONS, D), jnp.float32), 0.25, 1.75).astype(jnp.bfloat16),
        "proj_weight": gaussian(streams_of[6], (MEMBERS, SECTIONS, D, 3 * D), D ** -0.5, 0.5, ((0, 2), (1, 4))),
        "out_weight": gaussian(streams_of[7], (MEMBERS, SECTIONS, D, D), D ** -0.5, 0.5, ((0, 2), (1, 4))),
        "force_coef": gaussian(streams_of[8], (MEMBERS, SECTIONS, HEADS), 16.0, 48.0, ((0, 2), (1, 4))),
    }


def block_ref(h_in, gain, proj, outw, coef, pair, delta):
    hf = h_in.astype(jnp.float32)
    normed = (hf * lax.rsqrt(lax.optimization_barrier(jnp.mean(hf * hf, -1, keepdims=True)) + 1e-06) * gain.astype(jnp.float32)).astype(jnp.bfloat16)
    query = jnp.dot(normed, proj[:, :D], preferred_element_type=jnp.float32).astype(jnp.bfloat16)
    keyval = jnp.dot(normed, proj[:, D:], preferred_element_type=jnp.float32).astype(jnp.bfloat16)
    query3 = query.astype(jnp.float32).reshape(ATOMS, HEADS, HEAD_DIM)
    keys = keyval[:, :D].astype(jnp.float32).reshape(ATOMS, HEADS, HEAD_DIM)
    values = keyval[:, D:].astype(jnp.float32).reshape(ATOMS, HEADS, HEAD_DIM)
    scores = jnp.einsum('ahd,jhd->haj', query3, keys) / math.sqrt(HEAD_DIM)
    weights = jax.nn.sigmoid(scores) * pair[None]
    rounded = lax.optimization_barrier(weights.astype(jnp.bfloat16)).astype(jnp.float32)
    message = (jnp.einsum('haj,jhd->ahd', rounded, values) / NBR).reshape(ATOMS, D).astype(jnp.bfloat16)
    h_out = (hf + jnp.dot(message, outw, preferred_element_type=jnp.float32)).astype(jnp.bfloat16)
    pair_coef = jnp.einsum('h,haj->aj', coef.astype(jnp.float32), weights)
    force = jnp.einsum('aj,caj->ca', pair_coef, delta) / NBR
    return (h_out, force)

def frame_pairs(nbr, mask, pos):
    rows = jnp.broadcast_to(jnp.arange(ATOMS, dtype=jnp.int32)[:, None], (ATOMS, NBR))
    counts = jnp.zeros((ATOMS, ATOMS), jnp.float32).at[rows, nbr].add(mask.astype(jnp.float32))
    delta = pos[:, None, :] - pos[:, :, None]
    switch = 1.0 / (1.0 + 0.125 * lax.optimization_barrier(jnp.sum(delta * delta, 0)))
    return (counts * switch, delta)

def reference(positions, atom_types, neighbors, nbr_mask, type_table, norm_gain, proj_weight, out_weight, force_coef):

    def member_forces(member):

        def frame_force(frame):
            pair, delta = frame_pairs(neighbors[frame], nbr_mask[frame], positions[frame])
            h_cur = jnp.take(type_table[member], atom_types[frame], axis=0)
            total = jnp.zeros((3, ATOMS), jnp.float32)
            for blk in range(SECTIONS):
                h_cur, term = block_ref(h_cur, norm_gain[member, blk], proj_weight[member, blk], out_weight[member, blk], force_coef[member, blk], pair, delta)
                total = total + term
            return total
        return lax.map(frame_force, jnp.arange(MICRO, dtype=jnp.int32))
    forces = lax.map(member_forces, jnp.arange(MEMBERS, dtype=jnp.int32))
    mean_force = lax.optimization_barrier(jnp.mean(forces, 0))
    centered = forces - mean_force[None]
    atom_dev = jnp.sqrt(lax.optimization_barrier(jnp.mean(lax.optimization_barrier(jnp.sum(centered * centered, 2)), 0)))
    max_dev = lax.optimization_barrier(jnp.max(atom_dev, -1))
    return (atom_dev, max_dev, mean_force)
```

```python
import math

import jax
import jax.numpy as jnp
from jax import lax
from jax.experimental import pallas as pl
from jax.experimental.pallas import tpu as pltpu
from jax.sharding import PartitionSpec as P

F32 = jnp.float32
BF16 = jnp.bfloat16
EXTRA = 8
NIBBLES = 8
WROWS = 16


def dest(axis_size, index, r):
    if axis_size & (axis_size - 1) == 0:
        return index ^ r
    return (index + r) % axis_size


def source(axis_size, index, r):
    if axis_size & (axis_size - 1) == 0:
        return index ^ r
    return (index - r) % axis_size


def back(axis_size, index, g):
    if axis_size & (axis_size - 1) == 0:
        return index ^ g
    return (index - g) % axis_size


def exchange(x, axis, axis_size, r):
    if r == 0:
        return x
    return lax.ppermute(x, axis, [(i, dest(axis_size, i, r)) for i in range(axis_size)])


def pack_kernel(n_section, n_atoms, pos_ref, typ_ref, nbr_ref, mask_ref, *refs):
    frames = pos_ref.shape[0]
    per_section = frames // n_section
    outs, (nbr_v, mask_v, sems) = refs[:per_section], refs[per_section:]
    first = lax.axis_index("section") * per_section
    mine = lax.axis_index("atoms") % per_section
    copies = []
    for x in range(per_section):
        frame = first + dest(per_section, mine, x)
        a = pltpu.make_async_copy(nbr_ref.at[frame], nbr_v.at[x], sems.at[x, 0])
        b = pltpu.make_async_copy(mask_ref.at[frame], mask_v.at[x], sems.at[x, 1])
        a.start()
        b.start()
        copies.append((frame, a, b))
    for x, (frame, a, b) in enumerate(copies):
        a.wait()
        b.wait()
        slots = nbr_v.shape[2]
        count = nbr_v.shape[1]
        eff = jnp.where(mask_v[x] != 0, nbr_v[x], -1).astype(F32)
        outs[x][:slots, :] = jnp.transpose(eff)
        pos = pos_ref[frame]
        typ = typ_ref[pl.ds(frame, 1), :].astype(F32)
        outs[x][slots:, :] = jnp.concatenate(
            [pos, typ, jnp.zeros((EXTRA - 4, count), F32)], axis=0
        )


def histogram(list_ref, slice_id, slots, total):
    low = total // NIBBLES
    count = list_ref.shape[2]
    iota = lax.broadcasted_iota(jnp.int32, (low, count), 0)

    def chunk(c, acc):
        even, odd = acc
        eff = list_ref[slice_id, pl.ds(c * 8, 8), :]
        hi = jnp.floor((eff + 0.5) * (1.0 / low))
        lo = jnp.where(eff < 0, -1.0, eff - hi * low).astype(jnp.int32)
        weight = jnp.left_shift(1, 4 * jnp.maximum(hi, 0.0).astype(jnp.int32))
        nib = jnp.zeros((low, count), jnp.int32)
        for s in range(8):
            nib = nib + jnp.where(iota == lo[s : s + 1, :], weight[s : s + 1, :], 0)
        even = even + (nib & 0x0F0F0F0F)
        odd = odd + (lax.shift_right_logical(nib, 4) & 0x0F0F0F0F)
        return even, odd

    zero = jnp.zeros((low, count), jnp.int32)
    even, odd = lax.fori_loop(0, slots // 8, chunk, (zero, zero))
    rows = []
    for n in range(NIBBLES):
        acc = odd if n % 2 else even
        rows.append((lax.shift_right_logical(acc, 8 * (n // 2)) & 0xFF).astype(F32))
    return rows


def dot(a, b):
    return lax.dot_general(a, b, (((1,), (0,)), ((), ())), preferred_element_type=F32)


def dot_t(a, b):
    return lax.dot_general(a, b, (((0,), (0,)), ((), ())), preferred_element_type=F32)


def main_kernel(n_section, n_atoms, heads, *refs):
    lists_in = refs[:n_atoms]
    weights_in = refs[n_atoms : n_atoms + n_section]
    table_ref, out_ref, list_v, w_v, p_v, h_v, f_v = refs[n_atoms + n_section :]
    slots = list_v.shape[1] - EXTRA
    count = list_v.shape[2]
    total = n_atoms * count
    width = table_ref.shape[1]
    head_dim = width // heads
    low = total // NIBBLES
    a_idx = lax.axis_index("atoms")
    s_idx = lax.axis_index("section")
    for r in range(n_atoms):
        list_v[source(n_atoms, a_idx, r)] = lists_in[r][...]
    for r in range(n_section):
        w_v[source(n_section, s_idx, r)] = weights_in[r][...]

    extra = jnp.concatenate([list_v[b, slots:, :] for b in range(n_atoms)], axis=1)
    pos_col = jnp.transpose(extra)
    for b in range(n_atoms):
        rows = histogram(list_v, b, slots, total)
        for n in range(NIBBLES):
            part = pos_col[n * low : (n + 1) * low]
            dist = None
            for c in range(3):
                delta = part[:, c : c + 1] - extra[c : c + 1, b * count : (b + 1) * count]
                dist = delta * delta if dist is None else dist + delta * delta
            p_v[n * low : (n + 1) * low, b * count : (b + 1) * count] = (
                0.5 * rows[n] / (1.0 + 0.125 * dist)
            )

    types = extra[3:4, :].astype(jnp.int32)
    onehot = (lax.broadcasted_iota(jnp.int32, (table_ref.shape[0], total), 0) == types).astype(BF16)
    h_v[...] = dot_t(table_ref[...], onehot).astype(BF16).astype(F32)
    pos = extra[:3, :]
    pos_hi = pos.astype(BF16).astype(F32)
    pos_lo = pos - pos_hi
    tail = jnp.concatenate(
        [pos_hi, pos_lo, jnp.ones((1, total), F32), jnp.zeros((9, total), F32)], axis=0
    ).astype(BF16)
    f_v[...] = jnp.zeros_like(f_v)
    scale = 0.5 / math.sqrt(head_dim)
    tile = min(256, total)

    def block(b, carry):
        w = w_v[b]
        gain = jnp.transpose(
            jnp.broadcast_to(w[width : width + 1, :width].astype(F32), (width, width))
        )[:, :1]
        coef = w[width : width + 1, width : width + heads].astype(F32)
        h = h_v[...]
        norm = lax.rsqrt(jnp.mean(h * h, axis=0, keepdims=True) + 1e-06)
        x = (h * norm * gain).astype(BF16)
        wmat = w[:width]
        qkv = dot_t(wmat[:, : 3 * width], x)
        q = (qkv[:width] * scale).astype(BF16)
        k = jnp.transpose(qkv[width : 2 * width]).astype(BF16)
        v = qkv[2 * width :].astype(BF16)
        msgs = []
        for t in range(total // tile):
            lanes = slice(t * tile, (t + 1) * tile)
            p = p_v[:, lanes]
            parts = []
            force = None
            for hd in range(heads):
                rows = slice(hd * head_dim, (hd + 1) * head_dim)
                pieces = []
                if hd > 0:
                    pieces.append(jnp.zeros((hd * head_dim, tile), BF16))
                pieces.append(q[rows, lanes])
                if hd < heads - 1:
                    pieces.append(jnp.zeros(((heads - 1 - hd) * head_dim, tile), BF16))
                score = dot(k, jnp.concatenate(pieces, axis=0))
                g = (p * jnp.tanh(score) + p).astype(BF16)
                lhs = jnp.concatenate([v[rows], tail], axis=0)
                res = dot(lhs, g)
                parts.append(res[:head_dim])
                term = coef[:, hd : hd + 1] * res[head_dim : head_dim + 8]
                force = term if force is None else force + term
            f_v[:, lanes] = f_v[:, lanes] + force
            msgs.append(jnp.concatenate(parts, axis=0))
        msg = (jnp.concatenate(msgs, axis=1) / slots).astype(BF16)
        h_v[...] = (h + dot_t(wmat[:, 3 * width :], msg)).astype(BF16).astype(F32)
        return carry

    lax.fori_loop(0, n_section, block, 0)
    f = f_v[...]
    force = (f[0:3] + f[3:6] - pos * f[6:7]) / slots
    out_ref[...] = jnp.concatenate([force, jnp.zeros((5, total), F32)], axis=0)


def shards(n_member, n_section, n_atoms):
    def body(
        positions,
        atom_types,
        neighbors,
        nbr_mask,
        type_table,
        norm_gain,
        proj_weight,
        out_weight,
        force_coef,
    ):
        frames = positions.shape[0]
        per_section = frames // n_section
        count, slots = neighbors.shape[1:]
        total = count * n_atoms
        heads = force_coef.shape[-1]
        width = out_weight.shape[-1]
        any_spec = pl.BlockSpec(memory_space=pl.ANY)
        vmem = pl.BlockSpec(memory_space=pltpu.VMEM)

        own_w = jnp.concatenate([proj_weight[0, 0], out_weight[0, 0]], axis=1)
        row = jnp.concatenate(
            [norm_gain[0, 0], force_coef[0, 0], jnp.zeros((3 * width - heads,), BF16)]
        )
        own_w = jnp.concatenate(
            [own_w, jnp.broadcast_to(row[None], (WROWS, 4 * width))], axis=0
        )
        weights = [exchange(own_w, "section", n_section, r) for r in range(n_section)]

        packed = pl.pallas_call(
            lambda *refs: pack_kernel(n_section, n_atoms, *refs),
            out_shape=[jax.ShapeDtypeStruct((slots + EXTRA, count), F32)] * per_section,
            in_specs=[vmem, vmem, any_spec, any_spec],
            out_specs=[vmem] * per_section,
            scratch_shapes=[
                pltpu.VMEM((per_section, count, slots), jnp.int32),
                pltpu.VMEM((per_section, count, slots), jnp.int32),
                pltpu.SemaphoreType.DMA((per_section, 2)),
            ],
            name="pack",
        )(positions, atom_types, neighbors, nbr_mask)
        lists = [
            exchange(packed[r % per_section], "atoms", n_atoms, r) for r in range(n_atoms)
        ]

        force = pl.pallas_call(
            lambda *refs: main_kernel(n_section, n_atoms, heads, *refs),
            out_shape=jax.ShapeDtypeStruct((8, total), F32),
            in_specs=[vmem] * (n_atoms + n_section + 1),
            out_specs=vmem,
            scratch_shapes=[
                pltpu.VMEM((n_atoms, slots + EXTRA, count), F32),
                pltpu.VMEM((n_section, width + WROWS, 4 * width), BF16),
                pltpu.VMEM((total, total), F32),
                pltpu.VMEM((width, total), F32),
                pltpu.VMEM((8, total), F32),
            ],
            name="frame",
        )(*lists, *weights, type_table[0])

        others = [force[:3]] + [
            exchange(force, "member", n_member, r)[:3] for r in range(1, n_member)
        ]
        mean = sum(others) / n_member
        spread = sum(jnp.sum((f - mean) * (f - mean), 0, keepdims=True) for f in others)
        dev = jnp.sqrt(spread / n_member)
        result = jnp.concatenate([mean, dev, jnp.zeros((4, total), F32)], axis=0)
        mine = lax.axis_index("atoms") % per_section
        got = jnp.stack(
            [result] + [exchange(result, "atoms", n_atoms, r) for r in range(1, per_section)]
        )
        got = jnp.stack(
            [
                lax.dynamic_index_in_dim(got, back(per_section, mine, g), 0, keepdims=False)
                for g in range(per_section)
            ]
        )
        own = lax.dynamic_slice_in_dim(got, lax.axis_index("atoms") * count, count, 2)
        return own[:, 3], jnp.max(got[:, 3], -1), own[:, :3]

    return body


def solution(mesh):
    sizes = mesh.shape
    return jax.shard_map(
        shards(sizes["member"], sizes["section"], sizes["atoms"]),
        mesh=mesh,
        in_specs=(
            P(None, None, "atoms"),
            P(None, "atoms"),
            P(None, "atoms", None),
            P(None, "atoms", None),
            P("member", None, None),
            P("member", "section", None),
            P("member", "section", None, None),
            P("member", "section", None, None),
            P("member", "section", None),
        ),
        out_specs=(P("section", "atoms"), P("section"), P("section", None, "atoms")),
        check_vma=False,
    )
```

```python
import math

import jax
import jax.numpy as jnp
from jax import lax
from jax.experimental import pallas as pl
from jax.experimental.pallas import tpu as pltpu
from jax.sharding import PartitionSpec as P

F32 = jnp.float32
BF16 = jnp.bfloat16
EXTRA = 8
NIBBLES = 8
AHEAD = 6
LAG = 2
WROWS = 16
FRAME_PARAMS = pltpu.CompilerParams()


def dest(axis_size, index, r):
    if axis_size & (axis_size - 1) == 0:
        return index ^ r
    return (index + r) % axis_size


def source(axis_size, index, r):
    if axis_size & (axis_size - 1) == 0:
        return index ^ r
    return (index - r) % axis_size


def exchange(x, axis, axis_size, r):
    if r == 0:
        return x
    return lax.ppermute(x, axis, [(i, dest(axis_size, i, r)) for i in range(axis_size)])


def dot(a, b):
    return lax.dot_general(a, b, (((1,), (0,)), ((), ())), preferred_element_type=F32)


def pack_kernel(n_section, pos_ref, typ_ref, nbr_ref, mask_ref, proj_ref, outw_ref, *refs):
    gain_ref, coef_ref = refs[:2]
    frames = pos_ref.shape[1]
    per_section = frames // n_section
    outs, w_out = refs[2 : 2 + per_section], refs[2 + per_section]
    pos_v, typ_v, nbr_v, mask_v, gain_v, coef_v, sems = refs[3 + per_section :]
    first = lax.axis_index("section") * per_section
    mine = lax.axis_index("atoms") % per_section
    side = outw_ref.shape[0]
    small = [
        pltpu.make_async_copy(pos_ref, pos_v, sems.at[0]),
        pltpu.make_async_copy(typ_ref, typ_v, sems.at[1]),
    ]
    for c in small:
        c.start()
    lists = []
    for x in range(per_section):
        frame = first + dest(per_section, mine, x)
        a = pltpu.make_async_copy(nbr_ref.at[frame], nbr_v.at[x], sems.at[6 + 2 * x])
        b = pltpu.make_async_copy(mask_ref.at[frame], mask_v.at[x], sems.at[7 + 2 * x])
        a.start()
        b.start()
        lists.append((frame, a, b))
    weights = [
        pltpu.make_async_copy(proj_ref, w_out.at[:side, : 3 * side], sems.at[2]),
        pltpu.make_async_copy(outw_ref, w_out.at[:side, 3 * side :], sems.at[3]),
        pltpu.make_async_copy(gain_ref, gain_v, sems.at[4]),
        pltpu.make_async_copy(coef_ref, coef_v, sems.at[5]),
    ]
    for c in weights:
        c.start()
    for c in small:
        c.wait()
    for x, (frame, a, b) in enumerate(lists):
        a.wait()
        b.wait()
        slots = nbr_v.shape[2]
        count = nbr_v.shape[1]
        eff = jnp.where(mask_v[x] != 0, nbr_v[x], -1).astype(F32)
        outs[x][:slots, :] = jnp.transpose(eff)
        rows = [pos_v[c, pl.ds(frame, 1), :] for c in range(3)]
        rows.append(typ_v[pl.ds(frame, 1), :].astype(F32))
        rows.append(jnp.zeros((EXTRA - 4, count), F32))
        outs[x][slots:, :] = jnp.concatenate(rows, axis=0)
    for c in weights:
        c.wait()
    heads = coef_v.shape[1]
    row = jnp.concatenate(
        [gain_v[...], coef_v[...], jnp.zeros((1, 3 * side - heads), BF16)], axis=1
    )
    w_out[side:, :] = jnp.broadcast_to(row.astype(F32), (WROWS, 4 * side)).astype(BF16)


def slice_kernel(total, msg_ref, table_ref, cnt_ref, h_ref):
    slots = msg_ref.shape[0] - EXTRA
    count = msg_ref.shape[1]
    low = total // NIBBLES
    types = msg_ref[slots + 3 : slots + 4, :].astype(jnp.int32)
    iota_t = lax.broadcasted_iota(jnp.int32, (table_ref.shape[0], count), 0)
    onehot = (iota_t == types).astype(BF16)
    h_ref[...] = dot(jnp.transpose(table_ref[...]), onehot)
    iota = lax.broadcasted_iota(jnp.int32, (low, count), 0)

    def chunk(c, acc):
        even, odd = acc
        eff = msg_ref[pl.ds(c * 8, 8), :]
        hi = jnp.floor((eff + 0.5) * (1.0 / low))
        lo = jnp.where(eff < 0, -1.0, eff - hi * low).astype(jnp.int32)
        weight = jnp.left_shift(1, 4 * jnp.maximum(hi, 0.0).astype(jnp.int32))
        nib = None
        for s in range(8):
            one = jnp.where(iota == lo[s : s + 1, :], weight[s : s + 1, :], 0)
            nib = one if nib is None else nib + one
        even = even + (nib & 0x0F0F0F0F)
        odd = odd + (lax.shift_right_logical(nib, 4) & 0x0F0F0F0F)
        return even, odd

    zero = jnp.zeros((low, count), jnp.int32)
    even, odd = lax.fori_loop(0, slots // 8, chunk, (zero, zero))
    cnt_ref[:low, :] = even
    cnt_ref[low:, :] = odd


def frame_kernel(n_section, n_atoms, heads, slots, *refs):
    msgs, refs = refs[:n_atoms], refs[n_atoms:]
    counts, refs = refs[:n_atoms], refs[n_atoms:]
    embeds, refs = refs[:n_atoms], refs[n_atoms:]
    weights_in, refs = refs[:n_section], refs[n_section:]
    out_ref, ext_v, w_v, p_v = refs
    count = msgs[0].shape[1]
    total = n_atoms * count
    width = embeds[0].shape[0]
    head_dim = width // heads
    low = total // NIBBLES
    a_idx = lax.axis_index("atoms")
    s_idx = lax.axis_index("section")
    tile = max(count, min(256, total // 4))
    tiles = total // tile
    per_tile = tile // count
    group = max(1, 256 // tile)
    span = [slice(t * tile, (t + 1) * tile) for t in range(tiles)]

    for r in range(n_section):
        w = weights_in[r][...]
        side = w.shape[0] - WROWS
        gain = jnp.transpose(
            jnp.broadcast_to(w[side : side + 1, :side].astype(F32), (side, side))
        ).astype(BF16)
        w_v[source(n_section, s_idx, r)] = jnp.concatenate(
            [jnp.transpose(w[:side]), gain, w[side:, :side], w[side:, side : 2 * side]], axis=0
        )

    ext = [msgs[r][slots:, :] for r in range(n_atoms)]
    for r in range(n_atoms):
        ext_v[source(n_atoms, a_idx, r)] = ext[r]
    pos_col = jnp.concatenate([jnp.transpose(ext_v[b]) for b in range(n_atoms)], axis=0)
    pos = jnp.concatenate(ext, axis=1)[:3]
    pos_hi = pos.astype(BF16).astype(F32)
    tail = jnp.concatenate(
        [pos_hi, pos - pos_hi, jnp.ones((1, total), F32), jnp.zeros((9, total), F32)], axis=0
    ).astype(BF16)

    def pairs(r):
        lanes = slice(r * count, (r + 1) * count)
        for n in range(NIBBLES):
            acc = counts[r][low:, :] if n % 2 else counts[r][:low, :]
            hits = (lax.shift_right_logical(acc, 8 * (n // 2)) & 0xFF).astype(F32)
            part = pos_col[n * low : (n + 1) * low]
            dist = None
            for c in range(3):
                delta = part[:, c : c + 1] - ext[r][c : c + 1, :]
                dist = delta * delta if dist is None else dist + delta * delta
            p_v[n * low : (n + 1) * low, lanes] = 0.5 * hits / (1.0 + 0.125 * dist)

    scale = 0.5 / math.sqrt(head_dim)
    h = [
        jnp.concatenate(
            [embeds[r][...] for r in range(t * per_tile, (t + 1) * per_tile)], axis=1
        )
        for t in range(tiles)
    ]
    state = {}
    force = [None] * tiles
    results = {}
    zeros = {}

    def zero_rows(n):
        if n not in zeros:
            zeros[n] = jnp.zeros((n, tile), BF16)
        return zeros[n]

    def project(b, t):
        w = w_v[b]
        norm = lax.rsqrt(jnp.mean(h[t] * h[t], axis=0, keepdims=True) + 1e-06)
        x = (h[t] * norm * w[4 * width : 5 * width, :1].astype(F32)).astype(BF16)
        qkv = dot(w[: 3 * width, :width], x)
        k = jnp.transpose(qkv[width : 2 * width].astype(BF16))
        q = (qkv[:width] * scale).astype(BF16)
        v = qkv[2 * width :].astype(BF16)
        rhs = []
        for first in range(0, heads, group):
            cols = []
            for hd in range(first, first + group):
                rows = [q[hd * head_dim : (hd + 1) * head_dim]]
                if hd > 0:
                    rows.insert(0, zero_rows(hd * head_dim))
                if hd < heads - 1:
                    rows.append(zero_rows((heads - 1 - hd) * head_dim))
                cols.append(jnp.concatenate(rows, axis=0))
            rhs.append(jnp.concatenate(cols, axis=1))
        state[b, t] = rhs, k, v

    def score(b, t, jt, g):
        return dot(state[b, jt][1], state[b, t][0][g])

    def consume(unit, value):
        b, t, jt, g = unit
        p = jnp.concatenate(
            [
                p_v[pl.ds(source(n_atoms, a_idx, r) * count, count), span[t]]
                for r in range(jt * per_tile, (jt + 1) * per_tile)
            ],
            axis=0,
        )
        parts = []
        for i in range(group):
            parts.append(p * jnp.tanh(value[:, i * tile : (i + 1) * tile]) + p)
        return jnp.concatenate(parts, axis=1).astype(BF16)

    def message(unit, value):
        b, t, jt, g = unit
        rows = slice(g * group * head_dim, (g + 1) * group * head_dim)
        lhs = jnp.concatenate([state[b, jt][2][rows], tail[:, span[jt]]], axis=0)
        res = dot(lhs, value)
        for i in range(group):
            lanes = slice(i * tile, (i + 1) * tile)
            own = (
                res[i * head_dim : (i + 1) * head_dim, lanes],
                res[group * head_dim : group * head_dim + 8, lanes],
            )
            key = b, t, g * group + i
            if key in results:
                own = tuple(x + y for x, y in zip(results[key], own))
            results[key] = own

    def finish(b, t):
        w = w_v[b]
        parts = [results.pop((b, t, hd)) for hd in range(heads)]
        if b + 1 < n_section:
            msg = jnp.concatenate([part[0] for part in parts], axis=0) * (1.0 / slots)
            step = dot(w[3 * width : 4 * width], msg.astype(BF16))
            h[t] = (h[t] + step).astype(BF16).astype(F32)
            project(b + 1, t)
        coef = w[5 * width + WROWS : 5 * width + WROWS + 1, :heads].astype(F32)
        for hd, part in enumerate(parts):
            term = coef[:, hd : hd + 1] * part[1]
            force[t] = term if force[t] is None else force[t] + term

    last = tiles - 1
    order = [(t, jt) for t in range(last) for jt in range(last)]
    order += [(t, last) for t in range(last)]
    order += [(last, jt) for jt in range(tiles)]
    units = [
        (b, t, jt, g) for b in range(n_section) for t, jt in order for g in range(heads // group)
    ]
    left = {(b, t): tiles * (heads // group) for b in range(n_section) for t in range(tiles)}
    ready = set()
    pending, gated = [], []

    def retire():
        if pending:
            gate()
        if len(gated) > LAG or not pending:
            settle()

    def settle():
        unit, value = gated.pop(0)
        b, t = unit[:2]
        message(unit, value)
        left[b, t] -= 1
        if left[b, t] == 0:
            finish(b, t)

    def gate():
        unit, value = pending.pop(0)
        b, t = unit[:2]
        for r in range(t * per_tile, (t + 1) * per_tile):
            if r not in ready:
                ready.add(r)
                pairs(r)
        gated.append((unit, consume(unit, value)))

    for t in range(tiles):
        project(0, t)
    for unit in units:
        b, t, jt, g = unit
        while (b, t) not in state or (b, jt) not in state:
            retire()
        pending.append((unit, score(*unit)))
        while len(pending) > AHEAD:
            retire()
    while pending or gated:
        retire()

    f = jnp.concatenate(force, axis=1)
    out = (f[0:3] + f[3:6] - pos * f[6:7]) * (1.0 / slots)
    out_ref[...] = jnp.concatenate([out, jnp.zeros((5, total), F32)], axis=0)


def committee_kernel(*refs):
    forces, out_ref = [r[:3, :] for r in refs[:-1]], refs[-1]
    mean = sum(forces) * (1.0 / len(forces))
    spread = sum(jnp.sum((f - mean) * (f - mean), 0, keepdims=True) for f in forces)
    dev = jnp.sqrt(spread * (1.0 / len(forces)))
    out_ref[...] = jnp.concatenate([mean, dev, jnp.zeros((4, dev.shape[1]), F32)], axis=0)


def emit_kernel(n_atoms, count, *refs):
    ins, (dev_ref, max_ref, mean_ref) = refs[:-3], refs[-3:]
    per_section = len(ins)
    mine = lax.axis_index("atoms") % per_section
    for x in range(per_section):
        r = x if n_atoms & (n_atoms - 1) == 0 else (-x) % n_atoms
        frame = source(per_section, mine, x)
        mine_rows = ins[x][:4, r * count : (r + 1) * count]
        dev_ref[pl.ds(frame, 1), :] = mine_rows[3:4]
        for c in range(3):
            mean_ref[c, pl.ds(frame, 1), :] = mine_rows[c : c + 1]
        max_ref[frame] = jnp.max(ins[x][3:4, :])


def shards(n_member, n_section, n_atoms):
    def body(
        positions,
        atom_types,
        neighbors,
        nbr_mask,
        type_table,
        norm_gain,
        proj_weight,
        out_weight,
        force_coef,
    ):
        frames = positions.shape[0]
        per_section = frames // n_section
        count, slots = neighbors.shape[1:]
        total = count * n_atoms
        heads = force_coef.shape[-1]
        width = out_weight.shape[-1]
        any_spec = pl.BlockSpec(memory_space=pl.ANY)
        vmem = pl.BlockSpec(memory_space=pltpu.VMEM)
        smem = pl.BlockSpec(memory_space=pltpu.SMEM)
        shape = jax.ShapeDtypeStruct

        *packed, own_w = pl.pallas_call(
            lambda *refs: pack_kernel(n_section, *refs),
            out_shape=[shape((slots + EXTRA, count), F32)] * per_section
            + [shape((width + WROWS, 4 * width), BF16)],
            in_specs=[any_spec] * 8,
            out_specs=[vmem] * (per_section + 1),
            scratch_shapes=[
                pltpu.VMEM((3, frames, count), F32),
                pltpu.VMEM((frames, count), jnp.int32),
                pltpu.VMEM((per_section, count, slots), jnp.int32),
                pltpu.VMEM((per_section, count, slots), jnp.int32),
                pltpu.VMEM((1, width), BF16),
                pltpu.VMEM((1, heads), BF16),
                pltpu.SemaphoreType.DMA((6 + 2 * per_section,)),
            ],
            name="pack",
        )(
            jnp.transpose(positions, (1, 0, 2)),
            atom_types,
            neighbors,
            nbr_mask,
            proj_weight[0, 0],
            out_weight[0, 0],
            norm_gain[0],
            force_coef[0],
        )
        lists = [exchange(packed[r % per_section], "atoms", n_atoms, r) for r in range(n_atoms)]
        weights = [exchange(own_w, "section", n_section, r) for r in range(n_section)]

        def one_slice(msg):
            return pl.pallas_call(
                lambda *refs: slice_kernel(total, *refs),
                out_shape=[
                    shape((2 * (total // NIBBLES), count), jnp.int32),
                    shape((width, count), F32),
                ],
                in_specs=[vmem, vmem],
                out_specs=[vmem, vmem],
                name="slice",
            )(msg, type_table[0])

        slices = [one_slice(msg) for msg in lists]
        force = pl.pallas_call(
            lambda *refs: frame_kernel(n_section, n_atoms, heads, slots, *refs),
            out_shape=shape((8, total), F32),
            in_specs=[vmem] * (3 * n_atoms + n_section),
            out_specs=vmem,
            scratch_shapes=[
                pltpu.VMEM((n_atoms, EXTRA, count), F32),
                pltpu.VMEM((n_section, 5 * width + 2 * WROWS, width), BF16),
                pltpu.VMEM((total, total), F32),
            ],
            compiler_params=FRAME_PARAMS,
            name="frame",
        )(*lists, *[s[0] for s in slices], *[s[1] for s in slices], *weights)

        members = [exchange(force, "member", n_member, r) for r in range(n_member)]
        result = pl.pallas_call(
            committee_kernel,
            out_shape=shape((8, total), F32),
            in_specs=[vmem] * n_member,
            out_specs=vmem,
            name="committee",
        )(*members)
        got = [exchange(result, "atoms", n_atoms, r) for r in range(per_section)]
        atom_dev, max_dev, mean_force = pl.pallas_call(
            lambda *refs: emit_kernel(n_atoms, count, *refs),
            out_shape=[
                shape((per_section, count), F32),
                shape((per_section,), F32),
                shape((3, per_section, count), F32),
            ],
            in_specs=[vmem] * per_section,
            out_specs=[vmem, smem, vmem],
            name="emit",
        )(*got)
        return atom_dev, max_dev, jnp.transpose(mean_force, (1, 0, 2))

    return body


def solution(mesh):
    sizes = mesh.shape
    return jax.shard_map(
        shards(sizes["member"], sizes["section"], sizes["atoms"]),
        mesh=mesh,
        in_specs=(
            P(None, None, "atoms"),
            P(None, "atoms"),
            P(None, "atoms", None),
            P(None, "atoms", None),
            P("member", None, None),
            P("member", "section", None),
            P("member", "section", None, None),
            P("member", "section", None, None),
            P("member", "section", None),
        ),
        out_specs=(P("section", "atoms"), P("section"), P("section", None, "atoms")),
        check_vma=False,
    )
```

```python
import math

import jax
import jax.numpy as jnp
from jax import lax
from jax.experimental import pallas as pl
from jax.experimental.pallas import tpu as pltpu
from jax.sharding import PartitionSpec as P

F32 = jnp.float32
BF16 = jnp.bfloat16
EXTRA = 8
NIBBLES = 8
AHEAD = 6
LAG = 2
WROWS = 16
FRAME_PARAMS = pltpu.CompilerParams()


def dest(axis_size, index, r):
    if axis_size & (axis_size - 1) == 0:
        return index ^ r
    return (index + r) % axis_size


def source(axis_size, index, r):
    if axis_size & (axis_size - 1) == 0:
        return index ^ r
    return (index - r) % axis_size


def exchange(x, axis, axis_size, r):
    if r == 0:
        return x
    return lax.ppermute(x, axis, [(i, dest(axis_size, i, r)) for i in range(axis_size)])


def dot(a, b):
    return lax.dot_general(a, b, (((1,), (0,)), ((), ())), preferred_element_type=F32)


def pack_kernel(n_section, pos_ref, typ_ref, nbr_ref, mask_ref, proj_ref, outw_ref, *refs):
    gain_ref, coef_ref = refs[:2]
    frames = pos_ref.shape[1]
    per_section = frames // n_section
    outs, w_out = refs[2 : 2 + per_section], refs[2 + per_section]
    pos_v, typ_v, nbr_v, mask_v, gain_v, coef_v, sems = refs[3 + per_section :]
    first = lax.axis_index("section") * per_section
    mine = lax.axis_index("atoms") % per_section
    side = outw_ref.shape[0]
    small = [
        pltpu.make_async_copy(pos_ref, pos_v, sems.at[0]),
        pltpu.make_async_copy(typ_ref, typ_v, sems.at[1]),
    ]
    for c in small:
        c.start()
    lists = []
    for x in range(per_section):
        frame = first + dest(per_section, mine, x)
        a = pltpu.make_async_copy(nbr_ref.at[frame], nbr_v.at[x], sems.at[6 + 2 * x])
        b = pltpu.make_async_copy(mask_ref.at[frame], mask_v.at[x], sems.at[7 + 2 * x])
        a.start()
        b.start()
        lists.append((frame, a, b))
    weights = [
        pltpu.make_async_copy(proj_ref, w_out.at[:side, : 3 * side], sems.at[2]),
        pltpu.make_async_copy(outw_ref, w_out.at[:side, 3 * side :], sems.at[3]),
        pltpu.make_async_copy(gain_ref, gain_v, sems.at[4]),
        pltpu.make_async_copy(coef_ref, coef_v, sems.at[5]),
    ]
    for c in weights:
        c.start()
    for c in small:
        c.wait()
    for x, (frame, a, b) in enumerate(lists):
        a.wait()
        b.wait()
        slots = nbr_v.shape[2]
        count = nbr_v.shape[1]
        eff = jnp.where(mask_v[x] != 0, nbr_v[x], -1).astype(F32)
        outs[x][:slots, :] = jnp.transpose(eff)
        rows = [pos_v[c, pl.ds(frame, 1), :] for c in range(3)]
        rows.append(typ_v[pl.ds(frame, 1), :].astype(F32))
        rows.append(jnp.zeros((EXTRA - 4, count), F32))
        outs[x][slots:, :] = jnp.concatenate(rows, axis=0)
    for c in weights:
        c.wait()
    heads = coef_v.shape[1]
    row = jnp.concatenate(
        [gain_v[...], coef_v[...], jnp.zeros((1, 3 * side - heads), BF16)], axis=1
    )
    w_out[side:, :] = jnp.broadcast_to(row.astype(F32), (WROWS, 4 * side)).astype(BF16)


def count_slots(list_ref, slots, total, cnt_ref):
    count = list_ref.shape[1]
    low = total // NIBBLES
    iota = lax.broadcasted_iota(jnp.int32, (low, count), 0)
    cnt_ref[...] = jnp.zeros_like(cnt_ref)

    def chunk(c, carry):
        eff = list_ref[pl.ds(c * 8, 8), :]
        hi = jnp.floor((eff + 0.5) * (1.0 / low))
        lo = jnp.where(eff < 0, -1.0, eff - hi * low).astype(jnp.int32)
        weight = jnp.left_shift(1, 4 * jnp.maximum(hi, 0.0).astype(jnp.int32))
        nib = None
        for s in range(8):
            one = jnp.where(iota == lo[s : s + 1, :], weight[s : s + 1, :], 0)
            nib = one if nib is None else nib + one
        cnt_ref[:low, :] += nib & 0x0F0F0F0F
        cnt_ref[low:, :] += lax.shift_right_logical(nib, 4) & 0x0F0F0F0F
        return carry

    lax.fori_loop(0, slots // 8, chunk, 0)


def slice_kernel(total, msg_ref, cnt_ref):
    count_slots(msg_ref, msg_ref.shape[0] - EXTRA, total, cnt_ref)


def frame_kernel(n_section, n_atoms, heads, slots, *refs):
    msgs, refs = refs[:n_atoms], refs[n_atoms:]
    weights_in, refs = refs[:n_section], refs[n_section:]
    cnt_in, table_ref, out_ref, list_v, cnt_v, raw_v, table_v, ext_v, w_v, p_v, sems = refs
    count = msgs[0].shape[1]
    total = n_atoms * count
    width = table_ref.shape[1]
    head_dim = width // heads
    low = total // NIBBLES
    a_idx = lax.axis_index("atoms")
    s_idx = lax.axis_index("section")
    tile = max(count, min(256, total // 4))
    tiles = total // tile
    per_tile = tile // count
    group = max(1, 256 // tile)
    span = [slice(t * tile, (t + 1) * tile) for t in range(tiles)]

    own = pltpu.make_async_copy(
        msgs[0].at[slots:, :], list_v.at[0, slots:, :], sems.at[0]
    )
    list_copies = [own] + [
        pltpu.make_async_copy(msgs[r], list_v.at[r], sems.at[r]) for r in range(1, n_atoms)
    ]
    cnt_copy = pltpu.make_async_copy(cnt_in, cnt_v.at[0], sems.at[n_atoms])
    table_copy = pltpu.make_async_copy(table_ref, table_v, sems.at[n_atoms + 1])
    raw_copies = [
        pltpu.make_async_copy(weights_in[r], raw_v.at[r], sems.at[n_atoms + 2 + r])
        for r in range(n_section)
    ]
    for c in [*list_copies[1:], own, table_copy, cnt_copy, *raw_copies]:
        c.start()
    for r in range(1, n_atoms):
        list_copies[r].wait()
        count_slots(list_v.at[r], slots, total, cnt_v.at[r])
    own.wait()
    table_copy.wait()
    cnt_copy.wait()
    for c in raw_copies:
        c.wait()

    for r in range(n_section):
        w = raw_v[r]
        side = w.shape[0] - WROWS
        gain = jnp.transpose(
            jnp.broadcast_to(w[side : side + 1, :side].astype(F32), (side, side))
        ).astype(BF16)
        w_v[source(n_section, s_idx, r)] = jnp.concatenate(
            [jnp.transpose(w[:side]), gain, w[side:, :side], w[side:, side : 2 * side]], axis=0
        )

    ext = [list_v[r, slots:, :] for r in range(n_atoms)]
    for r in range(n_atoms):
        ext_v[source(n_atoms, a_idx, r)] = ext[r]
    pos_col = jnp.concatenate([jnp.transpose(ext_v[b]) for b in range(n_atoms)], axis=0)
    pos = jnp.concatenate(ext, axis=1)[:3]
    pos_hi = pos.astype(BF16).astype(F32)
    tail = jnp.concatenate(
        [pos_hi, pos - pos_hi, jnp.ones((1, total), F32), jnp.zeros((9, total), F32)], axis=0
    ).astype(BF16)
    types = jnp.concatenate(ext, axis=1)[3:4].astype(jnp.int32)
    iota_t = lax.broadcasted_iota(jnp.int32, (table_v.shape[0], total), 0)
    onehot = (iota_t == types).astype(BF16)
    embed = dot(jnp.transpose(table_v[...]), onehot)

    def pairs(r):
        lanes = slice(r * count, (r + 1) * count)
        for n in range(NIBBLES):
            acc = cnt_v[r, low:, :] if n % 2 else cnt_v[r, :low, :]
            hits = (lax.shift_right_logical(acc, 8 * (n // 2)) & 0xFF).astype(F32)
            part = pos_col[n * low : (n + 1) * low]
            dist = None
            for c in range(3):
                delta = part[:, c : c + 1] - ext[r][c : c + 1, :]
                dist = delta * delta if dist is None else dist + delta * delta
            p_v[n * low : (n + 1) * low, lanes] = 0.5 * hits / (1.0 + 0.125 * dist)

    scale = 0.5 / math.sqrt(head_dim)
    h = [embed[:, span[t]] for t in range(tiles)]
    state = {}
    force = [None] * tiles
    results = {}
    zeros = {}

    def zero_rows(n):
        if n not in zeros:
            zeros[n] = jnp.zeros((n, tile), BF16)
        return zeros[n]

    def project(b, t):
        w = w_v[b]
        norm = lax.rsqrt(jnp.mean(h[t] * h[t], axis=0, keepdims=True) + 1e-06)
        x = (h[t] * norm * w[4 * width : 5 * width, :1].astype(F32)).astype(BF16)
        qkv = dot(w[: 3 * width, :width], x)
        k = jnp.transpose(qkv[width : 2 * width].astype(BF16))
        q = (qkv[:width] * scale).astype(BF16)
        v = qkv[2 * width :].astype(BF16)
        rhs = []
        for first in range(0, heads, group):
            cols = []
            for hd in range(first, first + group):
                rows = [q[hd * head_dim : (hd + 1) * head_dim]]
                if hd > 0:
                    rows.insert(0, zero_rows(hd * head_dim))
                if hd < heads - 1:
                    rows.append(zero_rows((heads - 1 - hd) * head_dim))
                cols.append(jnp.concatenate(rows, axis=0))
            rhs.append(jnp.concatenate(cols, axis=1))
        state[b, t] = rhs, k, v

    def score(b, t, jt, g):
        return dot(state[b, jt][1], state[b, t][0][g])

    def consume(unit, value):
        b, t, jt, g = unit
        p = jnp.concatenate(
            [
                p_v[pl.ds(source(n_atoms, a_idx, r) * count, count), span[t]]
                for r in range(jt * per_tile, (jt + 1) * per_tile)
            ],
            axis=0,
        )
        parts = []
        for i in range(group):
            parts.append(p * jnp.tanh(value[:, i * tile : (i + 1) * tile]) + p)
        return jnp.concatenate(parts, axis=1).astype(BF16)

    def message(unit, value):
        b, t, jt, g = unit
        rows = slice(g * group * head_dim, (g + 1) * group * head_dim)
        lhs = jnp.concatenate([state[b, jt][2][rows], tail[:, span[jt]]], axis=0)
        res = dot(lhs, value)
        for i in range(group):
            lanes = slice(i * tile, (i + 1) * tile)
            own = (
                res[i * head_dim : (i + 1) * head_dim, lanes],
                res[group * head_dim : group * head_dim + 8, lanes],
            )
            key = b, t, g * group + i
            if key in results:
                own = tuple(x + y for x, y in zip(results[key], own))
            results[key] = own

    def finish(b, t):
        w = w_v[b]
        parts = [results.pop((b, t, hd)) for hd in range(heads)]
        if b + 1 < n_section:
            msg = jnp.concatenate([part[0] for part in parts], axis=0) * (1.0 / slots)
            step = dot(w[3 * width : 4 * width], msg.astype(BF16))
            h[t] = (h[t] + step).astype(BF16).astype(F32)
            project(b + 1, t)
        coef = w[5 * width + WROWS : 5 * width + WROWS + 1, :heads].astype(F32)
        for hd, part in enumerate(parts):
            term = coef[:, hd : hd + 1] * part[1]
            force[t] = term if force[t] is None else force[t] + term

    last = tiles - 1
    order = [(t, jt) for t in range(last) for jt in range(last)]
    order += [(t, last) for t in range(last)]
    order += [(last, jt) for jt in range(tiles)]
    units = [
        (b, t, jt, g) for b in range(n_section) for t, jt in order for g in range(heads // group)
    ]
    left = {(b, t): tiles * (heads // group) for b in range(n_section) for t in range(tiles)}
    ready = set()
    pending, gated = [], []

    def retire():
        if pending:
            gate()
        if len(gated) > LAG or not pending:
            settle()

    def settle():
        unit, value = gated.pop(0)
        b, t = unit[:2]
        message(unit, value)
        left[b, t] -= 1
        if left[b, t] == 0:
            finish(b, t)

    def gate():
        unit, value = pending.pop(0)
        b, t = unit[:2]
        for r in range(t * per_tile, (t + 1) * per_tile):
            if r not in ready:
                ready.add(r)
                pairs(r)
        gated.append((unit, consume(unit, value)))

    for t in range(tiles):
        project(0, t)
    for unit in units:
        b, t, jt, g = unit
        while (b, t) not in state or (b, jt) not in state:
            retire()
        pending.append((unit, score(*unit)))
        while len(pending) > AHEAD:
            retire()
    while pending or gated:
        retire()

    f = jnp.concatenate(force, axis=1)
    out = (f[0:3] + f[3:6] - pos * f[6:7]) * (1.0 / slots)
    out_ref[...] = jnp.concatenate([out, jnp.zeros((5, total), F32)], axis=0)


def emit_kernel(n_member, n_atoms, count, *refs):
    ins, (dev_ref, max_ref, mean_ref, members_v) = refs[:-4], refs[-4:]
    per_section = len(ins) // n_member
    mine = lax.axis_index("atoms") % per_section
    own = lax.axis_index("member")
    for x in range(per_section):
        for r in range(n_member):
            members_v[source(n_member, own, r)] = ins[x * n_member + r][...]
        forces = [members_v[m][:3] for m in range(n_member)]
        mean = sum(forces) * (1.0 / n_member)
        spread = sum(jnp.sum((f - mean) * (f - mean), 0, keepdims=True) for f in forces)
        dev = jnp.sqrt(spread * (1.0 / n_member))
        r = x if n_atoms & (n_atoms - 1) == 0 else (-x) % n_atoms
        lanes = slice(r * count, (r + 1) * count)
        frame = source(per_section, mine, x)
        dev_ref[pl.ds(frame, 1), :] = dev[:, lanes]
        for c in range(3):
            mean_ref[c, pl.ds(frame, 1), :] = mean[c : c + 1, lanes]
        max_ref[frame] = jnp.max(dev)


def shards(n_member, n_section, n_atoms):
    def body(
        positions,
        atom_types,
        neighbors,
        nbr_mask,
        type_table,
        norm_gain,
        proj_weight,
        out_weight,
        force_coef,
    ):
        frames = positions.shape[0]
        per_section = frames // n_section
        count, slots = neighbors.shape[1:]
        total = count * n_atoms
        heads = force_coef.shape[-1]
        width = out_weight.shape[-1]
        any_spec = pl.BlockSpec(memory_space=pl.ANY)
        vmem = pl.BlockSpec(memory_space=pltpu.VMEM)
        smem = pl.BlockSpec(memory_space=pltpu.SMEM)
        shape = jax.ShapeDtypeStruct

        *packed, own_w = pl.pallas_call(
            lambda *refs: pack_kernel(n_section, *refs),
            out_shape=[shape((slots + EXTRA, count), F32)] * per_section
            + [shape((width + WROWS, 4 * width), BF16)],
            in_specs=[any_spec] * 8,
            out_specs=[vmem] * (per_section + 1),
            scratch_shapes=[
                pltpu.VMEM((3, frames, count), F32),
                pltpu.VMEM((frames, count), jnp.int32),
                pltpu.VMEM((per_section, count, slots), jnp.int32),
                pltpu.VMEM((per_section, count, slots), jnp.int32),
                pltpu.VMEM((1, width), BF16),
                pltpu.VMEM((1, heads), BF16),
                pltpu.SemaphoreType.DMA((6 + 2 * per_section,)),
            ],
            name="pack",
        )(
            jnp.transpose(positions, (1, 0, 2)),
            atom_types,
            neighbors,
            nbr_mask,
            proj_weight[0, 0],
            out_weight[0, 0],
            norm_gain[0],
            force_coef[0],
        )
        lists = [exchange(packed[r % per_section], "atoms", n_atoms, r) for r in range(n_atoms)]
        weights = [exchange(own_w, "section", n_section, r) for r in range(n_section)]

        low = total // NIBBLES
        counted = pl.pallas_call(
            lambda *refs: slice_kernel(total, *refs),
            out_shape=shape((2 * low, count), jnp.int32),
            in_specs=[vmem],
            out_specs=vmem,
            name="slice",
        )(lists[0])
        n_sem = n_atoms + n_section + 2
        force = pl.pallas_call(
            lambda *refs: frame_kernel(n_section, n_atoms, heads, slots, *refs),
            out_shape=shape((8, total), F32),
            in_specs=[any_spec] * (n_atoms + n_section + 2),
            out_specs=vmem,
            scratch_shapes=[
                pltpu.VMEM((n_atoms, slots + EXTRA, count), F32),
                pltpu.VMEM((n_atoms, 2 * low, count), jnp.int32),
                pltpu.VMEM((n_section, width + WROWS, 4 * width), BF16),
                pltpu.VMEM(type_table.shape[1:], BF16),
                pltpu.VMEM((n_atoms, EXTRA, count), F32),
                pltpu.VMEM((n_section, 5 * width + 2 * WROWS, width), BF16),
                pltpu.VMEM((total, total), F32),
                pltpu.SemaphoreType.DMA((n_sem,)),
            ],
            compiler_params=FRAME_PARAMS,
            name="frame",
        )(*lists, *weights, counted, type_table[0])

        def joint(x, r):
            if x == 0 and r == 0:
                return force
            pairs = [
                (m * n_atoms + a, dest(n_member, m, r) * n_atoms + dest(n_atoms, a, x))
                for m in range(n_member)
                for a in range(n_atoms)
            ]
            return lax.ppermute(force, ("member", "atoms"), pairs)

        got = [joint(x, r) for x in range(per_section) for r in range(n_member)]
        atom_dev, max_dev, mean_force = pl.pallas_call(
            lambda *refs: emit_kernel(n_member, n_atoms, count, *refs),
            out_shape=[
                shape((per_section, count), F32),
                shape((per_section,), F32),
                shape((3, per_section, count), F32),
            ],
            in_specs=[vmem] * len(got),
            out_specs=[vmem, smem, vmem],
            scratch_shapes=[pltpu.VMEM((n_member, 8, total), F32)],
            name="emit",
        )(*got)
        return atom_dev, max_dev, jnp.transpose(mean_force, (1, 0, 2))

    return body


def solution(mesh):
    sizes = mesh.shape
    return jax.shard_map(
        shards(sizes["member"], sizes["section"], sizes["atoms"]),
        mesh=mesh,
        in_specs=(
            P(None, None, "atoms"),
            P(None, "atoms"),
            P(None, "atoms", None),
            P(None, "atoms", None),
            P("member", None, None),
            P("member", "section", None),
            P("member", "section", None, None),
            P("member", "section", None, None),
            P("member", "section", None),
        ),
        out_specs=(P("section", "atoms"), P("section"), P("section", None, "atoms")),
        check_vma=False,
    )
```

```python
import math

import jax
import jax.numpy as jnp
from jax import lax
from jax.experimental import pallas as pl
from jax.experimental.pallas import tpu as pltpu
from jax.sharding import PartitionSpec as P

F32 = jnp.float32
BF16 = jnp.bfloat16
EXTRA = 8
NIBBLES = 8
AHEAD = 6
LAG = 2
WROWS = 16
FRAME_PARAMS = pltpu.CompilerParams(
    vmem_limit_bytes=32 << 20,
)
SMALL_PARAMS = pltpu.CompilerParams(vmem_limit_bytes=8 << 20)


def dest(axis_size, index, r):
    if axis_size & (axis_size - 1) == 0:
        return index ^ r
    return (index + r) % axis_size


def source(axis_size, index, r):
    if axis_size & (axis_size - 1) == 0:
        return index ^ r
    return (index - r) % axis_size


def exchange(x, axis, axis_size, r):
    if r == 0:
        return x
    return lax.ppermute(x, axis, [(i, dest(axis_size, i, r)) for i in range(axis_size)])


def dot(a, b):
    return lax.dot_general(a, b, (((1,), (0,)), ((), ())), preferred_element_type=F32)


def pack_kernel(n_section, pos_ref, typ_ref, nbr_ref, mask_ref, proj_ref, outw_ref, *refs):
    gain_ref, coef_ref = refs[:2]
    frames = pos_ref.shape[1]
    per_section = frames // n_section
    outs, w_out = refs[2 : 2 + per_section], refs[2 + per_section]
    pos_v, typ_v, nbr_v, mask_v, gain_v, coef_v, sems = refs[3 + per_section :]
    first = lax.axis_index("section") * per_section
    mine = lax.axis_index("atoms") % per_section
    side = outw_ref.shape[0]
    small = [
        pltpu.make_async_copy(pos_ref, pos_v, sems.at[0]),
        pltpu.make_async_copy(typ_ref, typ_v, sems.at[1]),
    ]
    for c in small:
        c.start()
    lists = []
    for x in range(per_section):
        frame = first + dest(per_section, mine, x)
        a = pltpu.make_async_copy(nbr_ref.at[frame], nbr_v.at[x], sems.at[6 + 2 * x])
        b = pltpu.make_async_copy(mask_ref.at[frame], mask_v.at[x], sems.at[7 + 2 * x])
        a.start()
        b.start()
        lists.append((frame, a, b))
    weights = [
        pltpu.make_async_copy(proj_ref, w_out.at[:side, : 3 * side], sems.at[2]),
        pltpu.make_async_copy(outw_ref, w_out.at[:side, 3 * side :], sems.at[3]),
        pltpu.make_async_copy(gain_ref, gain_v, sems.at[4]),
        pltpu.make_async_copy(coef_ref, coef_v, sems.at[5]),
    ]
    for c in weights:
        c.start()
    for c in small:
        c.wait()
    for x, (frame, a, b) in enumerate(lists):
        a.wait()
        b.wait()
        slots = nbr_v.shape[2]
        count = nbr_v.shape[1]
        eff = jnp.where(mask_v[x] != 0, nbr_v[x], -1).astype(F32)
        outs[x][:slots, :] = jnp.transpose(eff)
        rows = [pos_v[c, pl.ds(frame, 1), :] for c in range(3)]
        rows.append(typ_v[pl.ds(frame, 1), :].astype(F32))
        rows.append(jnp.zeros((EXTRA - 4, count), F32))
        outs[x][slots:, :] = jnp.concatenate(rows, axis=0)
    for c in weights:
        c.wait()
    heads = coef_v.shape[1]
    row = jnp.concatenate(
        [gain_v[...], coef_v[...], jnp.zeros((1, 3 * side - heads), BF16)], axis=1
    )
    w_out[side:, :] = jnp.broadcast_to(row.astype(F32), (WROWS, 4 * side)).astype(BF16)


def count_slots(list_ref, slots, total, cnt_ref):
    count = list_ref.shape[1]
    low = total // NIBBLES
    iota = lax.broadcasted_iota(jnp.int32, (low, count), 0)
    cnt_ref[...] = jnp.zeros_like(cnt_ref)

    def chunk(c, carry):
        eff = list_ref[pl.ds(c * 8, 8), :]
        hi = jnp.floor((eff + 0.5) * (1.0 / low))
        lo = jnp.where(eff < 0, -1.0, eff - hi * low).astype(jnp.int32)
        weight = jnp.left_shift(1, 4 * jnp.maximum(hi, 0.0).astype(jnp.int32))
        nib = None
        for s in range(8):
            one = jnp.where(iota == lo[s : s + 1, :], weight[s : s + 1, :], 0)
            nib = one if nib is None else nib + one
        cnt_ref[:low, :] += nib & 0x0F0F0F0F
        cnt_ref[low:, :] += lax.shift_right_logical(nib, 4) & 0x0F0F0F0F
        return carry

    lax.fori_loop(0, slots // 8, chunk, 0)


def slice_kernel(total, msg_ref, cnt_ref):
    count_slots(msg_ref, msg_ref.shape[0] - EXTRA, total, cnt_ref)


def frame_kernel(n_section, n_atoms, heads, slots, *refs):
    msgs, refs = refs[:n_atoms], refs[n_atoms:]
    weights_in, refs = refs[:n_section], refs[n_section:]
    cnt_in, table_ref, out_ref, cnt_v, ext_v, w_v, p_v = refs
    count = msgs[0].shape[1]
    total = n_atoms * count
    width = table_ref.shape[1]
    head_dim = width // heads
    low = total // NIBBLES
    a_idx = lax.axis_index("atoms")
    s_idx = lax.axis_index("section")
    tile = max(count, min(256, total // 4))
    tiles = total // tile
    per_tile = tile // count
    group = max(1, 256 // tile)
    span = [slice(t * tile, (t + 1) * tile) for t in range(tiles)]

    for r in range(1, n_atoms):
        count_slots(msgs[r], slots, total, cnt_v.at[r])
    cnt_v[0] = cnt_in[...]

    for r in range(n_section):
        w = weights_in[r][...]
        side = w.shape[0] - WROWS
        gain = jnp.transpose(
            jnp.broadcast_to(w[side : side + 1, :side].astype(F32), (side, side))
        ).astype(BF16)
        w_v[source(n_section, s_idx, r)] = jnp.concatenate(
            [jnp.transpose(w[:side]), gain, w[side:, :side], w[side:, side : 2 * side]], axis=0
        )

    ext = [msgs[r][slots:, :] for r in range(n_atoms)]
    for r in range(n_atoms):
        ext_v[source(n_atoms, a_idx, r)] = ext[r]
    pos_col = jnp.concatenate([jnp.transpose(ext_v[b]) for b in range(n_atoms)], axis=0)
    pos = jnp.concatenate(ext, axis=1)[:3]
    pos_hi = pos.astype(BF16).astype(F32)
    tail = jnp.concatenate(
        [pos_hi, pos - pos_hi, jnp.ones((1, total), F32), jnp.zeros((9, total), F32)], axis=0
    ).astype(BF16)
    types = jnp.concatenate(ext, axis=1)[3:4].astype(jnp.int32)
    iota_t = lax.broadcasted_iota(jnp.int32, (table_ref.shape[0], total), 0)
    onehot = (iota_t == types).astype(BF16)
    embed = dot(jnp.transpose(table_ref[...]), onehot)

    def pairs(r):
        lanes = slice(r * count, (r + 1) * count)
        for n in range(NIBBLES):
            acc = cnt_v[r, low:, :] if n % 2 else cnt_v[r, :low, :]
            hits = (lax.shift_right_logical(acc, 8 * (n // 2)) & 0xFF).astype(F32)
            part = pos_col[n * low : (n + 1) * low]
            dist = None
            for c in range(3):
                delta = part[:, c : c + 1] - ext[r][c : c + 1, :]
                dist = delta * delta if dist is None else dist + delta * delta
            p_v[n * low : (n + 1) * low, lanes] = 0.5 * hits / (1.0 + 0.125 * dist)

    scale = 0.5 / math.sqrt(head_dim)
    h = [embed[:, span[t]] for t in range(tiles)]
    state = {}
    force = [None] * tiles
    results = {}
    zeros = {}

    def zero_rows(n):
        if n not in zeros:
            zeros[n] = jnp.zeros((n, tile), BF16)
        return zeros[n]

    def project(b, t):
        w = w_v[b]
        norm = lax.rsqrt(jnp.mean(h[t] * h[t], axis=0, keepdims=True) + 1e-06)
        x = (h[t] * norm * w[4 * width : 5 * width, :1].astype(F32)).astype(BF16)
        qkv = dot(w[: 3 * width, :width], x)
        k = jnp.transpose(qkv[width : 2 * width].astype(BF16))
        q = (qkv[:width] * scale).astype(BF16)
        v = qkv[2 * width :].astype(BF16)
        rhs = []
        for first in range(0, heads, group):
            cols = []
            for hd in range(first, first + group):
                rows = [q[hd * head_dim : (hd + 1) * head_dim]]
                if hd > 0:
                    rows.insert(0, zero_rows(hd * head_dim))
                if hd < heads - 1:
                    rows.append(zero_rows((heads - 1 - hd) * head_dim))
                cols.append(jnp.concatenate(rows, axis=0))
            rhs.append(jnp.concatenate(cols, axis=1))
        state[b, t] = rhs, k, v

    def score(b, t, jt, g):
        return dot(state[b, jt][1], state[b, t][0][g])

    def consume(unit, value):
        b, t, jt, g = unit
        p = jnp.concatenate(
            [
                p_v[pl.ds(source(n_atoms, a_idx, r) * count, count), span[t]]
                for r in range(jt * per_tile, (jt + 1) * per_tile)
            ],
            axis=0,
        )
        parts = []
        for i in range(group):
            parts.append(p * jnp.tanh(value[:, i * tile : (i + 1) * tile]) + p)
        return jnp.concatenate(parts, axis=1).astype(BF16)

    def message(unit, value):
        b, t, jt, g = unit
        rows = slice(g * group * head_dim, (g + 1) * group * head_dim)
        lhs = jnp.concatenate([state[b, jt][2][rows], tail[:, span[jt]]], axis=0)
        res = dot(lhs, value)
        for i in range(group):
            lanes = slice(i * tile, (i + 1) * tile)
            own = (
                res[i * head_dim : (i + 1) * head_dim, lanes],
                res[group * head_dim : group * head_dim + 8, lanes],
            )
            key = b, t, g * group + i
            if key in results:
                own = tuple(x + y for x, y in zip(results[key], own))
            results[key] = own

    def finish(b, t):
        w = w_v[b]
        parts = [results.pop((b, t, hd)) for hd in range(heads)]
        if b + 1 < n_section:
            msg = jnp.concatenate([part[0] for part in parts], axis=0) * (1.0 / slots)
            step = dot(w[3 * width : 4 * width], msg.astype(BF16))
            h[t] = (h[t] + step).astype(BF16).astype(F32)
            project(b + 1, t)
        coef = w[5 * width + WROWS : 5 * width + WROWS + 1, :heads].astype(F32)
        for hd, part in enumerate(parts):
            term = coef[:, hd : hd + 1] * part[1]
            force[t] = term if force[t] is None else force[t] + term

    last = tiles - 1
    order = [(t, jt) for t in range(last) for jt in range(last)]
    order += [(t, last) for t in range(last)]
    order += [(last, jt) for jt in range(tiles)]
    units = [
        (b, t, jt, g) for b in range(n_section) for t, jt in order for g in range(heads // group)
    ]
    left = {(b, t): tiles * (heads // group) for b in range(n_section) for t in range(tiles)}
    ready = set()
    pending, gated = [], []

    def retire():
        if pending:
            gate()
        if len(gated) > LAG or not pending:
            settle()

    def settle():
        unit, value = gated.pop(0)
        b, t = unit[:2]
        message(unit, value)
        left[b, t] -= 1
        if left[b, t] == 0:
            finish(b, t)

    def gate():
        unit, value = pending.pop(0)
        b, t = unit[:2]
        for r in range(t * per_tile, (t + 1) * per_tile):
            if r not in ready:
                ready.add(r)
                pairs(r)
        gated.append((unit, consume(unit, value)))

    for t in range(tiles):
        project(0, t)
    for unit in units:
        b, t, jt, g = unit
        while (b, t) not in state or (b, jt) not in state:
            retire()
        pending.append((unit, score(*unit)))
        while len(pending) > AHEAD:
            retire()
    while pending or gated:
        retire()

    f = jnp.concatenate(force, axis=1)
    out = (f[0:3] + f[3:6] - pos * f[6:7]) * (1.0 / slots)
    out_ref[...] = jnp.concatenate([out, jnp.zeros((5, total), F32)], axis=0)


def emit_kernel(n_member, n_atoms, count, *refs):
    ins, (dev_ref, max_ref, mean_ref, members_v) = refs[:-4], refs[-4:]
    per_section = len(ins) // n_member
    mine = lax.axis_index("atoms") % per_section
    own = lax.axis_index("member")
    for x in range(per_section):
        for r in range(n_member):
            members_v[source(n_member, own, r)] = ins[x * n_member + r][...]
        forces = [members_v[m][:3] for m in range(n_member)]
        mean = sum(forces) * (1.0 / n_member)
        spread = sum(jnp.sum((f - mean) * (f - mean), 0, keepdims=True) for f in forces)
        dev = jnp.sqrt(spread * (1.0 / n_member))
        r = x if n_atoms & (n_atoms - 1) == 0 else (-x) % n_atoms
        lanes = slice(r * count, (r + 1) * count)
        frame = source(per_section, mine, x)
        dev_ref[pl.ds(frame, 1), :] = dev[:, lanes]
        for c in range(3):
            mean_ref[c, pl.ds(frame, 1), :] = mean[c : c + 1, lanes]
        max_ref[frame] = jnp.max(dev)


def shards(n_member, n_section, n_atoms):
    def body(
        positions,
        atom_types,
        neighbors,
        nbr_mask,
        type_table,
        norm_gain,
        proj_weight,
        out_weight,
        force_coef,
    ):
        frames = positions.shape[0]
        per_section = frames // n_section
        count, slots = neighbors.shape[1:]
        total = count * n_atoms
        heads = force_coef.shape[-1]
        width = out_weight.shape[-1]
        any_spec = pl.BlockSpec(memory_space=pl.ANY)
        vmem = pl.BlockSpec(memory_space=pltpu.VMEM)
        smem = pl.BlockSpec(memory_space=pltpu.SMEM)
        shape = jax.ShapeDtypeStruct

        *packed, own_w = pl.pallas_call(
            lambda *refs: pack_kernel(n_section, *refs),
            out_shape=[shape((slots + EXTRA, count), F32)] * per_section
            + [shape((width + WROWS, 4 * width), BF16)],
            in_specs=[any_spec] * 8,
            out_specs=[vmem] * (per_section + 1),
            scratch_shapes=[
                pltpu.VMEM((3, frames, count), F32),
                pltpu.VMEM((frames, count), jnp.int32),
                pltpu.VMEM((per_section, count, slots), jnp.int32),
                pltpu.VMEM((per_section, count, slots), jnp.int32),
                pltpu.VMEM((1, width), BF16),
                pltpu.VMEM((1, heads), BF16),
                pltpu.SemaphoreType.DMA((6 + 2 * per_section,)),
            ],
            compiler_params=SMALL_PARAMS,
            name="pack",
        )(
            *[
                pltpu.with_memory_space_constraint(x, pltpu.HBM)
                for x in (
                    jnp.transpose(positions, (1, 0, 2)),
                    atom_types,
                    neighbors,
                    nbr_mask,
                    proj_weight[0, 0],
                    out_weight[0, 0],
                    norm_gain[0],
                    force_coef[0],
                )
            ]
        )
        lists = [exchange(packed[r % per_section], "atoms", n_atoms, r) for r in range(n_atoms)]
        weights = [exchange(own_w, "section", n_section, r) for r in range(n_section)]

        low = total // NIBBLES
        counted = pl.pallas_call(
            lambda *refs: slice_kernel(total, *refs),
            out_shape=shape((2 * low, count), jnp.int32),
            in_specs=[vmem],
            out_specs=vmem,
            compiler_params=SMALL_PARAMS,
            name="slice",
        )(lists[0])
        force = pl.pallas_call(
            lambda *refs: frame_kernel(n_section, n_atoms, heads, slots, *refs),
            out_shape=shape((8, total), F32),
            in_specs=[vmem] * (n_atoms + n_section + 2),
            out_specs=vmem,
            scratch_shapes=[
                pltpu.VMEM((n_atoms, 2 * low, count), jnp.int32),
                pltpu.VMEM((n_atoms, EXTRA, count), F32),
                pltpu.VMEM((n_section, 5 * width + 2 * WROWS, width), BF16),
                pltpu.VMEM((total, total), F32),
            ],
            compiler_params=FRAME_PARAMS,
            name="frame",
        )(*lists, *weights, counted, type_table[0])

        def joint(x, r):
            if x == 0 and r == 0:
                return force
            pairs = [
                (m * n_atoms + a, dest(n_member, m, r) * n_atoms + dest(n_atoms, a, x))
                for m in range(n_member)
                for a in range(n_atoms)
            ]
            return lax.ppermute(force, ("member", "atoms"), pairs)

        got = [joint(x, r) for x in range(per_section) for r in range(n_member)]
        atom_dev, max_dev, mean_force = pl.pallas_call(
            lambda *refs: emit_kernel(n_member, n_atoms, count, *refs),
            out_shape=[
                shape((per_section, count), F32),
                shape((per_section,), F32),
                shape((3, per_section, count), F32),
            ],
            in_specs=[vmem] * len(got),
            out_specs=[vmem, smem, vmem],
            scratch_shapes=[pltpu.VMEM((n_member, 8, total), F32)],
            compiler_params=SMALL_PARAMS,
            name="emit",
        )(*got)
        return atom_dev, max_dev, jnp.transpose(mean_force, (1, 0, 2))

    return body


def solution(mesh):
    sizes = mesh.shape
    return jax.shard_map(
        shards(sizes["member"], sizes["section"], sizes["atoms"]),
        mesh=mesh,
        in_specs=(
            P(None, None, "atoms"),
            P(None, "atoms"),
            P(None, "atoms", None),
            P(None, "atoms", None),
            P("member", None, None),
            P("member", "section", None),
            P("member", "section", None, None),
            P("member", "section", None, None),
            P("member", "section", None),
        ),
        out_specs=(P("section", "atoms"), P("section"), P("section", None, "atoms")),
        check_vma=False,
    )
```

```python
import math

import jax
import jax.numpy as jnp
from jax import lax
from jax.experimental import pallas as pl
from jax.experimental.pallas import tpu as pltpu
from jax.sharding import PartitionSpec as P

F32 = jnp.float32
BF16 = jnp.bfloat16
EXTRA = 8
NIBBLES = 8
AHEAD = 6
LAG = 2
WROWS = 16
FRAME_PARAMS = pltpu.CompilerParams(vmem_limit_bytes=32 << 20)
SMALL_PARAMS = pltpu.CompilerParams(vmem_limit_bytes=8 << 20)


def dest(axis_size, index, r):
    if axis_size & (axis_size - 1) == 0:
        return index ^ r
    return (index + r) % axis_size


def source(axis_size, index, r):
    if axis_size & (axis_size - 1) == 0:
        return index ^ r
    return (index - r) % axis_size


def exchange(x, axis, axis_size, r):
    if r == 0:
        return x
    return lax.ppermute(x, axis, [(i, dest(axis_size, i, r)) for i in range(axis_size)])


def dot(a, b):
    return lax.dot_general(a, b, (((1,), (0,)), ((), ())), preferred_element_type=F32)


def pack_kernel(n_section, pos_ref, typ_ref, nbr_ref, mask_ref, proj_ref, outw_ref, *refs):
    gain_ref, coef_ref = refs[:2]
    frames = pos_ref.shape[1]
    per_section = frames // n_section
    outs, w_out = refs[2 : 2 + per_section], refs[2 + per_section]
    pos_v, typ_v, nbr_v, mask_v, gain_v, coef_v, sems = refs[3 + per_section :]
    first = lax.axis_index("section") * per_section
    mine = lax.axis_index("atoms") % per_section
    side = outw_ref.shape[0]
    small = [
        pltpu.make_async_copy(pos_ref, pos_v, sems.at[0]),
        pltpu.make_async_copy(typ_ref, typ_v, sems.at[1]),
    ]
    for c in small:
        c.start()
    lists = []
    for x in range(per_section):
        frame = first + dest(per_section, mine, x)
        a = pltpu.make_async_copy(nbr_ref.at[frame], nbr_v.at[x], sems.at[6 + 2 * x])
        b = pltpu.make_async_copy(mask_ref.at[frame], mask_v.at[x], sems.at[7 + 2 * x])
        a.start()
        b.start()
        lists.append((frame, a, b))
    weights = [
        pltpu.make_async_copy(proj_ref, w_out.at[:side, : 3 * side], sems.at[2]),
        pltpu.make_async_copy(outw_ref, w_out.at[:side, 3 * side :], sems.at[3]),
        pltpu.make_async_copy(gain_ref, gain_v, sems.at[4]),
        pltpu.make_async_copy(coef_ref, coef_v, sems.at[5]),
    ]
    for c in weights:
        c.start()
    for c in small:
        c.wait()
    for x, (frame, a, b) in enumerate(lists):
        a.wait()
        b.wait()
        slots = nbr_v.shape[2]
        count = nbr_v.shape[1]
        eff = jnp.where(mask_v[x] != 0, nbr_v[x], -1).astype(F32)
        outs[x][:slots, :] = jnp.transpose(eff)
        rows = [pos_v[c, pl.ds(frame, 1), :] for c in range(3)]
        rows.append(typ_v[pl.ds(frame, 1), :].astype(F32))
        rows.append(jnp.zeros((EXTRA - 4, count), F32))
        outs[x][slots:, :] = jnp.concatenate(rows, axis=0)
    for c in weights:
        c.wait()
    heads = coef_v.shape[1]
    row = jnp.concatenate(
        [gain_v[...], coef_v[...], jnp.zeros((1, 3 * side - heads), BF16)], axis=1
    )
    w_out[side:, :] = jnp.broadcast_to(row.astype(F32), (WROWS, 4 * side)).astype(BF16)


def count_slots(list_ref, slots, total, cnt_ref):
    count = list_ref.shape[1]
    low = total // NIBBLES
    iota = lax.broadcasted_iota(jnp.int32, (low, count), 0)
    cnt_ref[...] = jnp.zeros_like(cnt_ref)

    def chunk(c, carry):
        eff = list_ref[pl.ds(c * 8, 8), :]
        hi = jnp.floor((eff + 0.5) * (1.0 / low))
        lo = jnp.where(eff < 0, -1.0, eff - hi * low).astype(jnp.int32)
        weight = jnp.left_shift(1, 4 * jnp.maximum(hi, 0.0).astype(jnp.int32))
        nib = None
        for s in range(8):
            one = jnp.where(iota == lo[s : s + 1, :], weight[s : s + 1, :], 0)
            nib = one if nib is None else nib + one
        cnt_ref[:low, :] += nib & 0x0F0F0F0F
        cnt_ref[low:, :] += lax.shift_right_logical(nib, 4) & 0x0F0F0F0F
        return carry

    lax.fori_loop(0, slots // 8, chunk, 0)


def slice_kernel(total, msg_ref, cnt_ref):
    count_slots(msg_ref, msg_ref.shape[0] - EXTRA, total, cnt_ref)


def frame_kernel(n_section, n_atoms, heads, slots, *refs):
    msgs, refs = refs[:n_atoms], refs[n_atoms:]
    weights_in, refs = refs[:n_section], refs[n_section:]
    cnt_v, refs = refs[:n_atoms], refs[n_atoms:]
    table_ref, out_ref, ext_v, w_v, p_v = refs
    count = msgs[0].shape[1]
    total = n_atoms * count
    width = table_ref.shape[1]
    head_dim = width // heads
    low = total // NIBBLES
    a_idx = lax.axis_index("atoms")
    s_idx = lax.axis_index("section")
    tile = max(count, min(256, total // 4))
    tiles = total // tile
    per_tile = tile // count
    group = max(1, 256 // tile)
    span = [slice(t * tile, (t + 1) * tile) for t in range(tiles)]

    for r in range(n_section):
        w = weights_in[r][...]
        side = w.shape[0] - WROWS
        gain = jnp.transpose(
            jnp.broadcast_to(w[side : side + 1, :side].astype(F32), (side, side))
        ).astype(BF16)
        w_v[source(n_section, s_idx, r)] = jnp.concatenate(
            [jnp.transpose(w[:side]), gain, w[side:, :side], w[side:, side : 2 * side]], axis=0
        )

    ext = [msgs[r][slots:, :] for r in range(n_atoms)]
    for r in range(n_atoms):
        ext_v[source(n_atoms, a_idx, r)] = ext[r]
    pos_col = jnp.concatenate([jnp.transpose(ext_v[b]) for b in range(n_atoms)], axis=0)
    pos = jnp.concatenate(ext, axis=1)[:3]
    pos_hi = pos.astype(BF16).astype(F32)
    tail = jnp.concatenate(
        [pos_hi, pos - pos_hi, jnp.ones((1, total), F32), jnp.zeros((9, total), F32)], axis=0
    ).astype(BF16)
    types = jnp.concatenate(ext, axis=1)[3:4].astype(jnp.int32)
    iota_t = lax.broadcasted_iota(jnp.int32, (table_ref.shape[0], total), 0)
    onehot = (iota_t == types).astype(BF16)
    embed = dot(jnp.transpose(table_ref[...]), onehot)

    def pairs(r):
        lanes = slice(r * count, (r + 1) * count)
        for n in range(NIBBLES):
            acc = cnt_v[r][low:, :] if n % 2 else cnt_v[r][:low, :]
            hits = (lax.shift_right_logical(acc, 8 * (n // 2)) & 0xFF).astype(F32)
            part = pos_col[n * low : (n + 1) * low]
            dist = None
            for c in range(3):
                delta = part[:, c : c + 1] - ext[r][c : c + 1, :]
                dist = delta * delta if dist is None else dist + delta * delta
            p_v[n * low : (n + 1) * low, lanes] = 0.5 * hits / (1.0 + 0.125 * dist)

    scale = 0.5 / math.sqrt(head_dim)
    h = [embed[:, span[t]] for t in range(tiles)]
    state = {}
    force = [None] * tiles
    results = {}
    zeros = {}

    def zero_rows(n):
        if n not in zeros:
            zeros[n] = jnp.zeros((n, tile), BF16)
        return zeros[n]

    def project(b, t):
        w = w_v[b]
        norm = lax.rsqrt(jnp.mean(h[t] * h[t], axis=0, keepdims=True) + 1e-06)
        x = (h[t] * norm * w[4 * width : 5 * width, :1].astype(F32)).astype(BF16)
        qkv = dot(w[: 3 * width, :width], x)
        k = jnp.transpose(qkv[width : 2 * width].astype(BF16))
        q = (qkv[:width] * scale).astype(BF16)
        v = qkv[2 * width :].astype(BF16)
        rhs = []
        for first in range(0, heads, group):
            cols = []
            for hd in range(first, first + group):
                rows = [q[hd * head_dim : (hd + 1) * head_dim]]
                if hd > 0:
                    rows.insert(0, zero_rows(hd * head_dim))
                if hd < heads - 1:
                    rows.append(zero_rows((heads - 1 - hd) * head_dim))
                cols.append(jnp.concatenate(rows, axis=0))
            rhs.append(jnp.concatenate(cols, axis=1))
        state[b, t] = rhs, k, v

    def score(b, t, jt, g):
        return dot(state[b, jt][1], state[b, t][0][g])

    def consume(unit, value):
        _, t, jt, _ = unit
        p = jnp.concatenate(
            [
                p_v[pl.ds(source(n_atoms, a_idx, r) * count, count), span[t]]
                for r in range(jt * per_tile, (jt + 1) * per_tile)
            ],
            axis=0,
        )
        parts = []
        for i in range(group):
            parts.append(p * jnp.tanh(value[:, i * tile : (i + 1) * tile]) + p)
        return jnp.concatenate(parts, axis=1).astype(BF16)

    def message(unit, value):
        b, t, jt, g = unit
        rows = slice(g * group * head_dim, (g + 1) * group * head_dim)
        lhs = jnp.concatenate([state[b, jt][2][rows], tail[:, span[jt]]], axis=0)
        res = dot(lhs, value)
        for i in range(group):
            lanes = slice(i * tile, (i + 1) * tile)
            own = (
                res[i * head_dim : (i + 1) * head_dim, lanes],
                res[group * head_dim : group * head_dim + 8, lanes],
            )
            key = b, t, g * group + i
            if key in results:
                own = tuple(x + y for x, y in zip(results[key], own))
            results[key] = own

    def finish(b, t):
        w = w_v[b]
        parts = [results.pop((b, t, hd)) for hd in range(heads)]
        if b + 1 < n_section:
            msg = jnp.concatenate([part[0] for part in parts], axis=0) * (1.0 / slots)
            step = dot(w[3 * width : 4 * width], msg.astype(BF16))
            h[t] = (h[t] + step).astype(BF16).astype(F32)
            project(b + 1, t)
        coef = w[5 * width + WROWS : 5 * width + WROWS + 1, :heads].astype(F32)
        for hd, part in enumerate(parts):
            term = coef[:, hd : hd + 1] * part[1]
            force[t] = term if force[t] is None else force[t] + term

    last = tiles - 1
    order = [(t, jt) for t in range(last) for jt in range(last)]
    order += [(t, last) for t in range(last)]
    order += [(last, jt) for jt in range(tiles)]
    units = [
        (b, t, jt, g) for b in range(n_section) for t, jt in order for g in range(heads // group)
    ]
    left = {(b, t): tiles * (heads // group) for b in range(n_section) for t in range(tiles)}
    ready = set()
    pending, gated = [], []

    def retire():
        if pending:
            gate()
        if len(gated) > LAG or not pending:
            settle()

    def settle():
        unit, value = gated.pop(0)
        b, t = unit[:2]
        message(unit, value)
        left[b, t] -= 1
        if left[b, t] == 0:
            finish(b, t)

    def gate():
        unit, value = pending.pop(0)
        _, t = unit[:2]
        for r in range(t * per_tile, (t + 1) * per_tile):
            if r not in ready:
                ready.add(r)
                pairs(r)
        gated.append((unit, consume(unit, value)))

    for t in range(tiles):
        project(0, t)
    for unit in units:
        b, t, jt, _ = unit
        while (b, t) not in state or (b, jt) not in state:
            retire()
        pending.append((unit, score(*unit)))
        while len(pending) > AHEAD:
            retire()
    while pending or gated:
        retire()

    f = jnp.concatenate(force, axis=1)
    out = (f[0:3] + f[3:6] - pos * f[6:7]) * (1.0 / slots)
    out_ref[...] = jnp.concatenate([out, jnp.zeros((5, total), F32)], axis=0)


def emit_kernel(n_member, n_atoms, count, *refs):
    ins, (dev_ref, max_ref, mean_ref, members_v) = refs[:-4], refs[-4:]
    per_section = len(ins) // n_member
    mine = lax.axis_index("atoms") % per_section
    own = lax.axis_index("member")
    for x in range(per_section):
        for r in range(n_member):
            members_v[source(n_member, own, r)] = ins[x * n_member + r][...]
        forces = [members_v[m][:3] for m in range(n_member)]
        mean = sum(forces) * (1.0 / n_member)
        spread = sum(jnp.sum((f - mean) * (f - mean), 0, keepdims=True) for f in forces)
        dev = jnp.sqrt(spread * (1.0 / n_member))
        r = x if n_atoms & (n_atoms - 1) == 0 else (-x) % n_atoms
        lanes = slice(r * count, (r + 1) * count)
        frame = source(per_section, mine, x)
        dev_ref[pl.ds(frame, 1), :] = dev[:, lanes]
        for c in range(3):
            mean_ref[c, pl.ds(frame, 1), :] = mean[c : c + 1, lanes]
        max_ref[frame] = jnp.max(dev)


def shards(n_member, n_section, n_atoms):
    def body(
        positions,
        atom_types,
        neighbors,
        nbr_mask,
        type_table,
        norm_gain,
        proj_weight,
        out_weight,
        force_coef,
    ):
        frames = positions.shape[0]
        per_section = frames // n_section
        count, slots = neighbors.shape[1:]
        total = count * n_atoms
        heads = force_coef.shape[-1]
        width = out_weight.shape[-1]
        any_spec = pl.BlockSpec(memory_space=pl.ANY)
        vmem = pl.BlockSpec(memory_space=pltpu.VMEM)
        smem = pl.BlockSpec(memory_space=pltpu.SMEM)
        shape = jax.ShapeDtypeStruct

        *packed, own_w = pl.pallas_call(
            lambda *refs: pack_kernel(n_section, *refs),
            out_shape=[shape((slots + EXTRA, count), F32)] * per_section
            + [shape((width + WROWS, 4 * width), BF16)],
            in_specs=[any_spec] * 8,
            out_specs=[vmem] * (per_section + 1),
            scratch_shapes=[
                pltpu.VMEM((3, frames, count), F32),
                pltpu.VMEM((frames, count), jnp.int32),
                pltpu.VMEM((per_section, count, slots), jnp.int32),
                pltpu.VMEM((per_section, count, slots), jnp.int32),
                pltpu.VMEM((1, width), BF16),
                pltpu.VMEM((1, heads), BF16),
                pltpu.SemaphoreType.DMA((6 + 2 * per_section,)),
            ],
            compiler_params=SMALL_PARAMS,
            name="pack",
        )(
            *[
                pltpu.with_memory_space_constraint(x, pltpu.HBM)
                for x in (
                    jnp.transpose(positions, (1, 0, 2)),
                    atom_types,
                    neighbors,
                    nbr_mask,
                    proj_weight[0, 0],
                    out_weight[0, 0],
                    norm_gain[0],
                    force_coef[0],
                )
            ]
        )
        lists = [exchange(packed[r % per_section], "atoms", n_atoms, r) for r in range(n_atoms)]
        weights = [exchange(own_w, "section", n_section, r) for r in range(n_section)]

        low = total // NIBBLES
        counted = [
            pl.pallas_call(
                lambda *refs: slice_kernel(total, *refs),
                out_shape=shape((2 * low, count), jnp.int32),
                in_specs=[vmem],
                out_specs=vmem,
                compiler_params=SMALL_PARAMS,
                name="slice",
            )(msg)
            for msg in lists
        ]
        force = pl.pallas_call(
            lambda *refs: frame_kernel(n_section, n_atoms, heads, slots, *refs),
            out_shape=shape((8, total), F32),
            in_specs=[vmem] * (2 * n_atoms + n_section + 1),
            out_specs=vmem,
            scratch_shapes=[
                pltpu.VMEM((n_atoms, EXTRA, count), F32),
                pltpu.VMEM((n_section, 5 * width + 2 * WROWS, width), BF16),
                pltpu.VMEM((total, total), F32),
            ],
            compiler_params=FRAME_PARAMS,
            name="frame",
        )(*lists, *weights, *counted, type_table[0])

        def joint(x, r):
            if x == 0 and r == 0:
                return force
            pairs = [
                (m * n_atoms + a, dest(n_member, m, r) * n_atoms + dest(n_atoms, a, x))
                for m in range(n_member)
                for a in range(n_atoms)
            ]
            return lax.ppermute(force, ("member", "atoms"), pairs)

        got = [joint(x, r) for x in range(per_section) for r in range(n_member)]
        atom_dev, max_dev, mean_force = pl.pallas_call(
            lambda *refs: emit_kernel(n_member, n_atoms, count, *refs),
            out_shape=[
                shape((per_section, count), F32),
                shape((per_section,), F32),
                shape((3, per_section, count), F32),
            ],
            in_specs=[vmem] * len(got),
            out_specs=[vmem, smem, vmem],
            scratch_shapes=[pltpu.VMEM((n_member, 8, total), F32)],
            compiler_params=SMALL_PARAMS,
            name="emit",
        )(*got)
        return atom_dev, max_dev, jnp.transpose(mean_force, (1, 0, 2))

    return body


def solution(mesh):
    sizes = mesh.shape
    return jax.shard_map(
        shards(sizes["member"], sizes["section"], sizes["atoms"]),
        mesh=mesh,
        in_specs=(
            P(None, None, "atoms"),
            P(None, "atoms"),
            P(None, "atoms", None),
            P(None, "atoms", None),
            P("member", None, None),
            P("member", "section", None),
            P("member", "section", None, None),
            P("member", "section", None, None),
            P("member", "section", None),
        ),
        out_specs=(P("section", "atoms"), P("section"), P("section", None, "atoms")),
        check_vma=False,
    )
```

```python
import math

import jax
import jax.numpy as jnp
from jax import lax
from jax.experimental import pallas as pl
from jax.experimental.pallas import tpu as pltpu
from jax.sharding import PartitionSpec as P

F32 = jnp.float32
BF16 = jnp.bfloat16
EXTRA = 8
NIBBLES = 8
AHEAD = 6
LAG = 2
WROWS = 16
FRAME_PARAMS = pltpu.CompilerParams(vmem_limit_bytes=32 << 20)
PAIRS_PARAMS = pltpu.CompilerParams(vmem_limit_bytes=16 << 20)
SMALL_PARAMS = pltpu.CompilerParams(vmem_limit_bytes=8 << 20)


def dest(axis_size, index, r):
    if axis_size & (axis_size - 1) == 0:
        return index ^ r
    return (index + r) % axis_size


def source(axis_size, index, r):
    if axis_size & (axis_size - 1) == 0:
        return index ^ r
    return (index - r) % axis_size


def exchange(x, axis, axis_size, r):
    if r == 0:
        return x
    return lax.ppermute(x, axis, [(i, dest(axis_size, i, r)) for i in range(axis_size)])


def dot(a, b):
    return lax.dot_general(a, b, (((1,), (0,)), ((), ())), preferred_element_type=F32)


def pack_kernel(n_section, pos_ref, typ_ref, nbr_ref, mask_ref, proj_ref, outw_ref, *refs):
    gain_ref, coef_ref = refs[:2]
    frames = pos_ref.shape[1]
    per_section = frames // n_section
    outs, w_out = refs[2 : 2 + per_section], refs[2 + per_section]
    pos_v, typ_v, nbr_v, mask_v, gain_v, coef_v, sems = refs[3 + per_section :]
    first = lax.axis_index("section") * per_section
    mine = lax.axis_index("atoms") % per_section
    side = outw_ref.shape[0]
    small = [
        pltpu.make_async_copy(pos_ref, pos_v, sems.at[0]),
        pltpu.make_async_copy(typ_ref, typ_v, sems.at[1]),
    ]
    for c in small:
        c.start()
    lists = []
    for x in range(per_section):
        frame = first + dest(per_section, mine, x)
        a = pltpu.make_async_copy(nbr_ref.at[frame], nbr_v.at[x], sems.at[6 + 2 * x])
        b = pltpu.make_async_copy(mask_ref.at[frame], mask_v.at[x], sems.at[7 + 2 * x])
        a.start()
        b.start()
        lists.append((frame, a, b))
    weights = [
        pltpu.make_async_copy(proj_ref, w_out.at[:side, : 3 * side], sems.at[2]),
        pltpu.make_async_copy(outw_ref, w_out.at[:side, 3 * side :], sems.at[3]),
        pltpu.make_async_copy(gain_ref, gain_v, sems.at[4]),
        pltpu.make_async_copy(coef_ref, coef_v, sems.at[5]),
    ]
    for c in weights:
        c.start()
    for c in small:
        c.wait()
    for x, (frame, a, b) in enumerate(lists):
        a.wait()
        b.wait()
        slots = nbr_v.shape[2]
        count = nbr_v.shape[1]
        eff = jnp.where(mask_v[x] != 0, nbr_v[x], -1).astype(F32)
        outs[x][:slots, :] = jnp.transpose(eff)
        rows = [pos_v[c, pl.ds(frame, 1), :] for c in range(3)]
        rows.append(typ_v[pl.ds(frame, 1), :].astype(F32))
        rows.append(jnp.zeros((EXTRA - 4, count), F32))
        outs[x][slots:, :] = jnp.concatenate(rows, axis=0)
    for c in weights:
        c.wait()
    heads = coef_v.shape[1]
    row = jnp.concatenate(
        [gain_v[...], coef_v[...], jnp.zeros((1, 3 * side - heads), BF16)], axis=1
    )
    w_out[side:, :] = jnp.broadcast_to(row.astype(F32), (WROWS, 4 * side)).astype(BF16)


def count_slots(list_ref, slots, total, cnt_ref):
    count = list_ref.shape[1]
    low = total // NIBBLES
    iota = lax.broadcasted_iota(jnp.int32, (low, count), 0)
    cnt_ref[...] = jnp.zeros_like(cnt_ref)

    def chunk(c, carry):
        eff = list_ref[pl.ds(c * 8, 8), :]
        hi = jnp.floor((eff + 0.5) * (1.0 / low))
        lo = jnp.where(eff < 0, -1.0, eff - hi * low).astype(jnp.int32)
        weight = jnp.left_shift(1, 4 * jnp.maximum(hi, 0.0).astype(jnp.int32))
        nib = None
        for s in range(8):
            one = jnp.where(iota == lo[s : s + 1, :], weight[s : s + 1, :], 0)
            nib = one if nib is None else nib + one
        cnt_ref[:low, :] += nib & 0x0F0F0F0F
        cnt_ref[low:, :] += lax.shift_right_logical(nib, 4) & 0x0F0F0F0F
        return carry

    lax.fori_loop(0, slots // 8, chunk, 0)


def slice_kernel(total, msg_ref, cnt_ref):
    count_slots(msg_ref, msg_ref.shape[0] - EXTRA, total, cnt_ref)


def pairs_kernel(n_atoms, *refs):
    msgs, cnt_v = refs[:n_atoms], refs[n_atoms : 2 * n_atoms]
    table_ref, p_ref, h_ref, ext_v = refs[2 * n_atoms :]
    slots = msgs[0].shape[0] - EXTRA
    count = msgs[0].shape[1]
    total = n_atoms * count
    low = total // NIBBLES
    a_idx = lax.axis_index("atoms")
    ext = [msgs[r][slots:, :] for r in range(n_atoms)]
    types = jnp.concatenate(ext, axis=1)[3:4].astype(jnp.int32)
    iota_t = lax.broadcasted_iota(jnp.int32, (table_ref.shape[0], total), 0)
    onehot = (iota_t == types).astype(BF16)
    h_ref[...] = dot(jnp.transpose(table_ref[...]), onehot)
    for r in range(n_atoms):
        ext_v[source(n_atoms, a_idx, r)] = ext[r]
    pos_col = jnp.concatenate([jnp.transpose(ext_v[b]) for b in range(n_atoms)], axis=0)
    for n in range(NIBBLES):
        part = pos_col[n * low : (n + 1) * low]
        cols = [jnp.broadcast_to(part[:, c : c + 1], (low, count)) for c in range(3)]
        for r in range(n_atoms):
            acc = cnt_v[r][low:, :] if n % 2 else cnt_v[r][:low, :]
            hits = (lax.shift_right_logical(acc, 8 * (n // 2)) & 0xFF).astype(F32)
            dist = None
            for c in range(3):
                delta = cols[c] - ext[r][c : c + 1, :]
                dist = delta * delta if dist is None else dist + delta * delta
            p_ref[n * low : (n + 1) * low, r * count : (r + 1) * count] = hits / (
                2.0 + 0.25 * dist
            )


def frame_kernel(n_section, n_atoms, heads, slots, *refs):
    msgs, refs = refs[:n_atoms], refs[n_atoms:]
    weights_in, refs = refs[:n_section], refs[n_section:]
    p_v, embed_ref, out_ref, w_v = refs
    count = msgs[0].shape[1]
    total = n_atoms * count
    width = embed_ref.shape[0]
    head_dim = width // heads
    a_idx = lax.axis_index("atoms")
    s_idx = lax.axis_index("section")
    tile = max(count, min(256, total // 4))
    tiles = total // tile
    per_tile = tile // count
    group = max(1, 256 // tile)
    span = [slice(t * tile, (t + 1) * tile) for t in range(tiles)]
    for r in range(n_section):
        w_v[source(n_section, s_idx, r)] = weights_in[r][...]
    pos = jnp.concatenate([msgs[r][slots:, :] for r in range(n_atoms)], axis=1)[:3]
    pos_hi = pos.astype(BF16).astype(F32)
    tail = jnp.concatenate(
        [pos_hi, pos - pos_hi, jnp.ones((1, total), F32), jnp.zeros((9, total), F32)], axis=0
    ).astype(BF16)

    scale = 0.5 / math.sqrt(head_dim)
    h = [embed_ref[:, span[t]] for t in range(tiles)]
    params = {}

    def load(b):
        w = w_v[b]
        row = w[width:]
        gain = jnp.transpose(jnp.broadcast_to(row[:1, :width].astype(F32), (width, width)))
        coef = row[:1, width : width + heads].astype(F32)
        params[b] = jnp.transpose(w[:width]), gain, coef

    state = {}
    force = [None] * tiles
    results = {}
    zeros = {}

    def zero_rows(n):
        if n not in zeros:
            zeros[n] = jnp.zeros((n, tile), BF16)
        return zeros[n]

    def project(b, t):
        if b not in params:
            load(b)
        w, gain, _ = params[b]
        norm = lax.rsqrt(jnp.mean(h[t] * h[t], axis=0, keepdims=True) + 1e-06)
        x = (h[t] * norm * gain[:, :1]).astype(BF16)
        qkv = dot(w[: 3 * width], x)
        k = jnp.transpose(qkv[width : 2 * width].astype(BF16))
        q = (qkv[:width] * scale).astype(BF16)
        v = qkv[2 * width :].astype(BF16)
        rhs = []
        for first in range(0, heads, group):
            cols = []
            for hd in range(first, first + group):
                rows = [q[hd * head_dim : (hd + 1) * head_dim]]
                if hd > 0:
                    rows.insert(0, zero_rows(hd * head_dim))
                if hd < heads - 1:
                    rows.append(zero_rows((heads - 1 - hd) * head_dim))
                cols.append(jnp.concatenate(rows, axis=0))
            rhs.append(jnp.concatenate(cols, axis=1))
        state[b, t] = rhs, k, v

    def score(b, t, jt, g):
        return dot(state[b, jt][1], state[b, t][0][g])

    def consume(unit, value):
        _, t, jt, _ = unit
        p = jnp.concatenate(
            [
                p_v[pl.ds(source(n_atoms, a_idx, r) * count, count), span[t]]
                for r in range(jt * per_tile, (jt + 1) * per_tile)
            ],
            axis=0,
        )
        parts = []
        for i in range(group):
            parts.append(p * jnp.tanh(value[:, i * tile : (i + 1) * tile]) + p)
        return jnp.concatenate(parts, axis=1).astype(BF16)

    def message(unit, value):
        b, t, jt, g = unit
        rows = slice(g * group * head_dim, (g + 1) * group * head_dim)
        lhs = jnp.concatenate([state[b, jt][2][rows], tail[:, span[jt]]], axis=0)
        res = dot(lhs, value)
        for i in range(group):
            lanes = slice(i * tile, (i + 1) * tile)
            own = (
                res[i * head_dim : (i + 1) * head_dim, lanes],
                res[group * head_dim : group * head_dim + 8, lanes],
            )
            key = b, t, g * group + i
            if key in results:
                own = tuple(x + y for x, y in zip(results[key], own))
            results[key] = own

    def finish(b, t):
        w, _, coef = params[b]
        parts = [results.pop((b, t, hd)) for hd in range(heads)]
        if b + 1 < n_section:
            msg = jnp.concatenate([part[0] for part in parts], axis=0) * (1.0 / slots)
            step = dot(w[3 * width :], msg.astype(BF16))
            h[t] = (h[t] + step).astype(BF16).astype(F32)
            project(b + 1, t)
        for hd, part in enumerate(parts):
            term = coef[:, hd : hd + 1] * part[1]
            force[t] = term if force[t] is None else force[t] + term

    last = tiles - 1
    order = [(t, jt) for t in range(last) for jt in range(last)]
    order += [(t, last) for t in range(last)]
    order += [(last, jt) for jt in range(tiles)]
    units = [
        (b, t, jt, g) for b in range(n_section) for t, jt in order for g in range(heads // group)
    ]
    left = {(b, t): tiles * (heads // group) for b in range(n_section) for t in range(tiles)}
    pending, gated = [], []

    def retire():
        if pending:
            gate()
        if len(gated) > LAG or not pending:
            settle()

    def settle():
        unit, value = gated.pop(0)
        b, t = unit[:2]
        message(unit, value)
        left[b, t] -= 1
        if left[b, t] == 0:
            finish(b, t)

    def gate():
        unit, value = pending.pop(0)
        gated.append((unit, consume(unit, value)))

    for t in range(tiles):
        project(0, t)
    for unit in units:
        b, t, jt, _ = unit
        while (b, t) not in state or (b, jt) not in state:
            retire()
        pending.append((unit, score(*unit)))
        while len(pending) > AHEAD:
            retire()
    while pending or gated:
        retire()

    f = jnp.concatenate(force, axis=1)
    out = (f[0:3] + f[3:6] - pos * f[6:7]) * (1.0 / slots)
    out_ref[...] = jnp.concatenate([out, jnp.zeros((5, total), F32)], axis=0)


def emit_kernel(n_member, n_atoms, count, *refs):
    ins, (dev_ref, max_ref, mean_ref, members_v) = refs[:-4], refs[-4:]
    per_section = len(ins) // n_member
    mine = lax.axis_index("atoms") % per_section
    own = lax.axis_index("member")
    for x in range(per_section):
        for r in range(n_member):
            members_v[source(n_member, own, r)] = ins[x * n_member + r][...]
        forces = [members_v[m][:3] for m in range(n_member)]
        mean = sum(forces) * (1.0 / n_member)
        spread = sum(jnp.sum((f - mean) * (f - mean), 0, keepdims=True) for f in forces)
        dev = jnp.sqrt(spread * (1.0 / n_member))
        r = x if n_atoms & (n_atoms - 1) == 0 else (-x) % n_atoms
        lanes = slice(r * count, (r + 1) * count)
        frame = source(per_section, mine, x)
        dev_ref[pl.ds(frame, 1), :] = dev[:, lanes]
        for c in range(3):
            mean_ref[c, pl.ds(frame, 1), :] = mean[c : c + 1, lanes]
        max_ref[frame] = jnp.max(dev)


def shards(n_member, n_section, n_atoms):
    def body(
        positions,
        atom_types,
        neighbors,
        nbr_mask,
        type_table,
        norm_gain,
        proj_weight,
        out_weight,
        force_coef,
    ):
        frames = positions.shape[0]
        per_section = frames // n_section
        count, slots = neighbors.shape[1:]
        total = count * n_atoms
        heads = force_coef.shape[-1]
        width = out_weight.shape[-1]
        any_spec = pl.BlockSpec(memory_space=pl.ANY)
        vmem = pl.BlockSpec(memory_space=pltpu.VMEM)
        smem = pl.BlockSpec(memory_space=pltpu.SMEM)
        shape = jax.ShapeDtypeStruct

        *packed, own_w = pl.pallas_call(
            lambda *refs: pack_kernel(n_section, *refs),
            out_shape=[shape((slots + EXTRA, count), F32)] * per_section
            + [shape((width + WROWS, 4 * width), BF16)],
            in_specs=[any_spec] * 8,
            out_specs=[vmem] * (per_section + 1),
            scratch_shapes=[
                pltpu.VMEM((3, frames, count), F32),
                pltpu.VMEM((frames, count), jnp.int32),
                pltpu.VMEM((per_section, count, slots), jnp.int32),
                pltpu.VMEM((per_section, count, slots), jnp.int32),
                pltpu.VMEM((1, width), BF16),
                pltpu.VMEM((1, heads), BF16),
                pltpu.SemaphoreType.DMA((6 + 2 * per_section,)),
            ],
            compiler_params=SMALL_PARAMS,
            name="pack",
        )(
            *[
                pltpu.with_memory_space_constraint(x, pltpu.HBM)
                for x in (
                    jnp.transpose(positions, (1, 0, 2)),
                    atom_types,
                    neighbors,
                    nbr_mask,
                    proj_weight[0, 0],
                    out_weight[0, 0],
                    norm_gain[0],
                    force_coef[0],
                )
            ]
        )
        lists = [exchange(packed[r % per_section], "atoms", n_atoms, r) for r in range(n_atoms)]
        weights = [exchange(own_w, "section", n_section, r) for r in range(n_section)]

        low = total // NIBBLES
        counted = [
            pl.pallas_call(
                lambda *refs: slice_kernel(total, *refs),
                out_shape=shape((2 * low, count), jnp.int32),
                in_specs=[vmem],
                out_specs=vmem,
                compiler_params=SMALL_PARAMS,
                name="slice",
            )(msg)
            for msg in lists
        ]
        pair, embed = pl.pallas_call(
            lambda *refs: pairs_kernel(n_atoms, *refs),
            out_shape=[shape((total, total), F32), shape((width, total), F32)],
            in_specs=[vmem] * (2 * n_atoms + 1),
            out_specs=[vmem, vmem],
            scratch_shapes=[pltpu.VMEM((n_atoms, EXTRA, count), F32)],
            compiler_params=PAIRS_PARAMS,
            name="pairs",
        )(*lists, *counted, type_table[0])
        force = pl.pallas_call(
            lambda *refs: frame_kernel(n_section, n_atoms, heads, slots, *refs),
            out_shape=shape((8, total), F32),
            in_specs=[vmem] * (n_atoms + n_section + 2),
            out_specs=vmem,
            scratch_shapes=[pltpu.VMEM((n_section, width + WROWS, 4 * width), BF16)],
            compiler_params=FRAME_PARAMS,
            name="frame",
        )(*lists, *weights, pair, embed)

        def joint(x, r):
            if x == 0 and r == 0:
                return force
            pairs = [
                (m * n_atoms + a, dest(n_member, m, r) * n_atoms + dest(n_atoms, a, x))
                for m in range(n_member)
                for a in range(n_atoms)
            ]
            return lax.ppermute(force, ("member", "atoms"), pairs)

        got = [joint(x, r) for x in range(per_section) for r in range(n_member)]
        atom_dev, max_dev, mean_force = pl.pallas_call(
            lambda *refs: emit_kernel(n_member, n_atoms, count, *refs),
            out_shape=[
                shape((per_section, count), F32),
                shape((per_section,), F32),
                shape((3, per_section, count), F32),
            ],
            in_specs=[vmem] * len(got),
            out_specs=[vmem, smem, vmem],
            scratch_shapes=[pltpu.VMEM((n_member, 8, total), F32)],
            compiler_params=SMALL_PARAMS,
            name="emit",
        )(*got)
        return atom_dev, max_dev, jnp.transpose(mean_force, (1, 0, 2))

    return body


def solution(mesh):
    sizes = mesh.shape
    return jax.shard_map(
        shards(sizes["member"], sizes["section"], sizes["atoms"]),
        mesh=mesh,
        in_specs=(
            P(None, None, "atoms"),
            P(None, "atoms"),
            P(None, "atoms", None),
            P(None, "atoms", None),
            P("member", None, None),
            P("member", "section", None),
            P("member", "section", None, None),
            P("member", "section", None, None),
            P("member", "section", None),
        ),
        out_specs=(P("section", "atoms"), P("section"), P("section", None, "atoms")),
        check_vma=False,
    )
```

```python
import math

import jax
import jax.numpy as jnp
from jax import lax
from jax.experimental import pallas as pl
from jax.experimental.pallas import tpu as pltpu
from jax.sharding import PartitionSpec as P

F32 = jnp.float32
BF16 = jnp.bfloat16
EXTRA = 8
NIBBLES = 8
AHEAD = 2
LAG = 2
WROWS = 16
FRAME_PARAMS = pltpu.CompilerParams(vmem_limit_bytes=32 << 20)
PAIRS_PARAMS = pltpu.CompilerParams(vmem_limit_bytes=16 << 20)
SMALL_PARAMS = pltpu.CompilerParams(vmem_limit_bytes=8 << 20)


def dest(axis_size, index, r):
    if axis_size & (axis_size - 1) == 0:
        return index ^ r
    return (index + r) % axis_size


def source(axis_size, index, r):
    if axis_size & (axis_size - 1) == 0:
        return index ^ r
    return (index - r) % axis_size


def exchange(x, axis, axis_size, r):
    if r == 0:
        return x
    return lax.ppermute(x, axis, [(i, dest(axis_size, i, r)) for i in range(axis_size)])


def dot(a, b):
    return lax.dot_general(a, b, (((1,), (0,)), ((), ())), preferred_element_type=F32)


def pack_kernel(n_section, pos_ref, typ_ref, nbr_ref, mask_ref, proj_ref, outw_ref, *refs):
    gain_ref, coef_ref = refs[:2]
    frames = pos_ref.shape[1]
    per_section = frames // n_section
    outs, w_out = refs[2 : 2 + per_section], refs[2 + per_section]
    pos_v, typ_v, nbr_v, mask_v, gain_v, coef_v, sems = refs[3 + per_section :]
    first = lax.axis_index("section") * per_section
    mine = lax.axis_index("atoms") % per_section
    side = outw_ref.shape[0]
    small = [
        pltpu.make_async_copy(pos_ref, pos_v, sems.at[0]),
        pltpu.make_async_copy(typ_ref, typ_v, sems.at[1]),
    ]
    for c in small:
        c.start()
    lists = []
    for x in range(per_section):
        frame = first + dest(per_section, mine, x)
        a = pltpu.make_async_copy(nbr_ref.at[frame], nbr_v.at[x], sems.at[6 + 2 * x])
        b = pltpu.make_async_copy(mask_ref.at[frame], mask_v.at[x], sems.at[7 + 2 * x])
        a.start()
        b.start()
        lists.append((frame, a, b))
    weights = [
        pltpu.make_async_copy(proj_ref, w_out.at[:side, : 3 * side], sems.at[2]),
        pltpu.make_async_copy(outw_ref, w_out.at[:side, 3 * side :], sems.at[3]),
        pltpu.make_async_copy(gain_ref, gain_v, sems.at[4]),
        pltpu.make_async_copy(coef_ref, coef_v, sems.at[5]),
    ]
    for c in weights:
        c.start()
    for c in small:
        c.wait()
    for x, (frame, a, b) in enumerate(lists):
        a.wait()
        b.wait()
        slots = nbr_v.shape[2]
        count = nbr_v.shape[1]
        eff = jnp.where(mask_v[x] != 0, nbr_v[x], -1).astype(F32)
        outs[x][:slots, :] = jnp.transpose(eff)
        rows = [pos_v[c, pl.ds(frame, 1), :] for c in range(3)]
        rows.append(typ_v[pl.ds(frame, 1), :].astype(F32))
        rows.append(jnp.zeros((EXTRA - 4, count), F32))
        outs[x][slots:, :] = jnp.concatenate(rows, axis=0)
    for c in weights:
        c.wait()
    heads = coef_v.shape[1]
    row = jnp.concatenate(
        [gain_v[...], coef_v[...], jnp.zeros((1, 3 * side - heads), BF16)], axis=1
    )
    w_out[side:, :] = jnp.broadcast_to(row.astype(F32), (WROWS, 4 * side)).astype(BF16)


def count_slots(list_ref, slots, total, cnt_ref):
    count = list_ref.shape[1]
    low = total // NIBBLES
    iota = lax.broadcasted_iota(jnp.int32, (low, count), 0)
    cnt_ref[...] = jnp.zeros_like(cnt_ref)

    def chunk(c, carry):
        eff = list_ref[pl.ds(c * 8, 8), :]
        hi = jnp.floor((eff + 0.5) * (1.0 / low))
        lo = jnp.where(eff < 0, -1.0, eff - hi * low).astype(jnp.int32)
        weight = jnp.left_shift(1, 4 * jnp.maximum(hi, 0.0).astype(jnp.int32))
        nib = None
        for s in range(8):
            one = jnp.where(iota == lo[s : s + 1, :], weight[s : s + 1, :], 0)
            nib = one if nib is None else nib + one
        cnt_ref[:low, :] += nib & 0x0F0F0F0F
        cnt_ref[low:, :] += lax.shift_right_logical(nib, 4) & 0x0F0F0F0F
        return carry

    lax.fori_loop(0, slots // 8, chunk, 0)


def slice_kernel(total, msg_ref, cnt_ref):
    count_slots(msg_ref, msg_ref.shape[0] - EXTRA, total, cnt_ref)


def pairs_kernel(n_atoms, *refs):
    msgs, cnt_v = refs[:n_atoms], refs[n_atoms : 2 * n_atoms]
    table_ref, p_ref, h_ref, ext_v = refs[2 * n_atoms :]
    slots = msgs[0].shape[0] - EXTRA
    count = msgs[0].shape[1]
    total = n_atoms * count
    low = total // NIBBLES
    a_idx = lax.axis_index("atoms")
    ext = [msgs[r][slots:, :] for r in range(n_atoms)]
    types = jnp.concatenate(ext, axis=1)[3:4].astype(jnp.int32)
    iota_t = lax.broadcasted_iota(jnp.int32, (table_ref.shape[0], total), 0)
    onehot = (iota_t == types).astype(BF16)
    h_ref[...] = dot(jnp.transpose(table_ref[...]), onehot)
    for r in range(n_atoms):
        ext_v[source(n_atoms, a_idx, r)] = ext[r]
    pos_col = jnp.concatenate([jnp.transpose(ext_v[b]) for b in range(n_atoms)], axis=0)
    for n in range(NIBBLES):
        part = pos_col[n * low : (n + 1) * low]
        cols = [jnp.broadcast_to(part[:, c : c + 1], (low, count)) for c in range(3)]
        for r in range(n_atoms):
            acc = cnt_v[r][low:, :] if n % 2 else cnt_v[r][:low, :]
            hits = (lax.shift_right_logical(acc, 8 * (n // 2)) & 0xFF).astype(F32)
            dist = None
            for c in range(3):
                delta = cols[c] - ext[r][c : c + 1, :]
                dist = delta * delta if dist is None else dist + delta * delta
            p_ref[n * low : (n + 1) * low, r * count : (r + 1) * count] = hits / (
                2.0 + 0.25 * dist
            )


def frame_kernel(n_section, n_atoms, heads, slots, *refs):
    msgs, refs = refs[:n_atoms], refs[n_atoms:]
    weights_in, refs = refs[:n_section], refs[n_section:]
    p_v, embed_ref, out_ref, w_v = refs
    count = msgs[0].shape[1]
    total = n_atoms * count
    width = embed_ref.shape[0]
    head_dim = width // heads
    a_idx = lax.axis_index("atoms")
    s_idx = lax.axis_index("section")
    tile = 256 if total % 256 == 0 else count
    tiles = total // tile
    per_tile = tile // count
    group = max(1, 256 // tile)
    span = [slice(t * tile, (t + 1) * tile) for t in range(tiles)]
    for r in range(n_section):
        w_v[source(n_section, s_idx, r)] = weights_in[r][...]
    pos = jnp.concatenate([msgs[r][slots:, :] for r in range(n_atoms)], axis=1)[:3]
    pos_hi = pos.astype(BF16).astype(F32)
    tail = jnp.concatenate(
        [pos_hi, pos - pos_hi, jnp.ones((1, total), F32), jnp.zeros((9, total), F32)], axis=0
    ).astype(BF16)

    scale = 0.5 / math.sqrt(head_dim)
    h = [embed_ref[:, span[t]] for t in range(tiles)]
    params = {}

    def load(b):
        w = w_v[b]
        row = w[width:]
        gain = jnp.transpose(jnp.broadcast_to(row[:1, :width].astype(F32), (width, width)))
        coef = row[:1, width : width + heads].astype(F32)
        params[b] = jnp.transpose(w[:width]), gain, coef

    state = {}
    force = [None] * tiles
    results = {}
    zeros = {}

    def zero_rows(n):
        if n not in zeros:
            zeros[n] = jnp.zeros((n, tile), BF16)
        return zeros[n]

    def project(b, t):
        if b not in params:
            load(b)
        w, gain, _ = params[b]
        norm = lax.rsqrt(jnp.mean(h[t] * h[t], axis=0, keepdims=True) + 1e-06)
        x = (h[t] * norm * gain[:, :1]).astype(BF16)
        k = jnp.transpose(dot(w[width : 2 * width], x).astype(BF16))
        q = dot(w[:width], x).astype(BF16).astype(F32) * scale
        q_hi = q.astype(BF16)
        q_lo = (q - q_hi.astype(F32)).astype(BF16)
        v = None
        if b + 1 < n_section:
            v = dot(w[2 * width : 3 * width], x).astype(BF16)
        rhs = []
        for first in range(0, heads, group):
            cols = []
            for hd in range(first, first + group):
                rows = []
                for term in (q_hi, q_lo):
                    if hd > 0:
                        rows.append(zero_rows(hd * head_dim))
                    rows.append(term[hd * head_dim : (hd + 1) * head_dim])
                    if hd < heads - 1:
                        rows.append(zero_rows((heads - 1 - hd) * head_dim))
                cols.append(jnp.concatenate(rows, axis=0))
            rhs.append(jnp.concatenate(cols, axis=1))
        k = jnp.concatenate([k, k], axis=1)
        state[b, t] = rhs, k, v

    def score(b, t, jt, g):
        return dot(state[b, jt][1], state[b, t][0][g])

    def consume(unit, value):
        _, t, jt, _ = unit
        p = jnp.concatenate(
            [
                p_v[pl.ds(source(n_atoms, a_idx, r) * count, count), span[t]]
                for r in range(jt * per_tile, (jt + 1) * per_tile)
            ],
            axis=0,
        )
        parts = []
        for i in range(group):
            parts.append(p * jnp.tanh(value[:, i * tile : (i + 1) * tile]) + p)
        return jnp.concatenate(parts, axis=1).astype(BF16)

    def message(unit, value):
        b, t, jt, g = unit
        lhs, base = tail[:, span[jt]], 0
        if b + 1 < n_section:
            base = group * head_dim
            rows = slice(g * base, (g + 1) * base)
            lhs = jnp.concatenate([state[b, jt][2][rows], lhs], axis=0)
        res = dot(lhs, value)
        for i in range(group):
            lanes = slice(i * tile, (i + 1) * tile)
            own = (
                res[base : base + 8, lanes],
                *([res[i * head_dim : (i + 1) * head_dim, lanes]] if base else []),
            )
            key = b, t, g * group + i
            if key in results:
                own = tuple(x + y for x, y in zip(results[key], own))
            results[key] = own

    def finish(b, t):
        w, _, coef = params[b]
        parts = [results.pop((b, t, hd)) for hd in range(heads)]
        if b + 1 < n_section:
            msg = jnp.concatenate([part[1] for part in parts], axis=0) * (1.0 / slots)
            step = dot(w[3 * width :], msg.astype(BF16))
            h[t] = (h[t] + step).astype(BF16).astype(F32)
            project(b + 1, t)
        for hd, part in enumerate(parts):
            term = coef[:, hd : hd + 1] * part[0]
            force[t] = term if force[t] is None else force[t] + term

    last = tiles - 1
    order = [(t, jt) for t in range(last) for jt in range(last)]
    order += [(t, last) for t in range(last)]
    order += [(last, jt) for jt in range(tiles)]
    units = [
        (b, t, jt, g) for b in range(n_section) for t, jt in order for g in range(heads // group)
    ]
    left = {(b, t): tiles * (heads // group) for b in range(n_section) for t in range(tiles)}
    pending, gated = [], []

    def retire():
        if pending:
            gate()
        if len(gated) > LAG or not pending:
            settle()

    def settle():
        unit, value = gated.pop(0)
        b, t = unit[:2]
        message(unit, value)
        left[b, t] -= 1
        if left[b, t] == 0:
            finish(b, t)

    def gate():
        unit, value = pending.pop(0)
        gated.append((unit, consume(unit, value)))

    for t in range(tiles):
        project(0, t)
    for unit in units:
        b, t, jt, _ = unit
        while (b, t) not in state or (b, jt) not in state:
            retire()
        pending.append((unit, score(*unit)))
        while len(pending) > AHEAD:
            retire()
    while pending or gated:
        retire()

    f = jnp.concatenate(force, axis=1)
    out = (f[0:3] + f[3:6] - pos * f[6:7]) * (1.0 / slots)
    out_ref[...] = jnp.concatenate([out, jnp.zeros((5, total), F32)], axis=0)


def emit_kernel(n_member, n_atoms, count, *refs):
    ins, (dev_ref, max_ref, mean_ref, members_v) = refs[:-4], refs[-4:]
    per_section = len(ins) // n_member
    mine = lax.axis_index("atoms") % per_section
    own = lax.axis_index("member")
    for x in range(per_section):
        for r in range(n_member):
            members_v[source(n_member, own, r)] = ins[x * n_member + r][...]
        forces = [members_v[m][:3] for m in range(n_member)]
        mean = sum(forces) * (1.0 / n_member)
        spread = sum(jnp.sum((f - mean) * (f - mean), 0, keepdims=True) for f in forces)
        dev = jnp.sqrt(spread * (1.0 / n_member))
        r = x if n_atoms & (n_atoms - 1) == 0 else (-x) % n_atoms
        lanes = slice(r * count, (r + 1) * count)
        frame = source(per_section, mine, x)
        dev_ref[pl.ds(frame, 1), :] = dev[:, lanes]
        for c in range(3):
            mean_ref[c, pl.ds(frame, 1), :] = mean[c : c + 1, lanes]
        max_ref[frame] = jnp.max(dev)


def shards(n_member, n_section, n_atoms):
    def body(
        positions,
        atom_types,
        neighbors,
        nbr_mask,
        type_table,
        norm_gain,
        proj_weight,
        out_weight,
        force_coef,
    ):
        frames = positions.shape[0]
        per_section = frames // n_section
        count, slots = neighbors.shape[1:]
        total = count * n_atoms
        heads = force_coef.shape[-1]
        width = out_weight.shape[-1]
        any_spec = pl.BlockSpec(memory_space=pl.ANY)
        vmem = pl.BlockSpec(memory_space=pltpu.VMEM)
        smem = pl.BlockSpec(memory_space=pltpu.SMEM)
        shape = jax.ShapeDtypeStruct

        *packed, own_w = pl.pallas_call(
            lambda *refs: pack_kernel(n_section, *refs),
            out_shape=[shape((slots + EXTRA, count), F32)] * per_section
            + [shape((width + WROWS, 4 * width), BF16)],
            in_specs=[any_spec] * 8,
            out_specs=[vmem] * (per_section + 1),
            scratch_shapes=[
                pltpu.VMEM((3, frames, count), F32),
                pltpu.VMEM((frames, count), jnp.int32),
                pltpu.VMEM((per_section, count, slots), jnp.int32),
                pltpu.VMEM((per_section, count, slots), jnp.int32),
                pltpu.VMEM((1, width), BF16),
                pltpu.VMEM((1, heads), BF16),
                pltpu.SemaphoreType.DMA((6 + 2 * per_section,)),
            ],
            compiler_params=SMALL_PARAMS,
            name="pack",
        )(
            *[
                pltpu.with_memory_space_constraint(x, pltpu.HBM)
                for x in (
                    jnp.transpose(positions, (1, 0, 2)),
                    atom_types,
                    neighbors,
                    nbr_mask,
                    proj_weight[0, 0],
                    out_weight[0, 0],
                    norm_gain[0],
                    force_coef[0],
                )
            ]
        )
        lists = [exchange(packed[r % per_section], "atoms", n_atoms, r) for r in range(n_atoms)]
        weights = [exchange(own_w, "section", n_section, r) for r in range(n_section)]

        low = total // NIBBLES
        counted = [
            pl.pallas_call(
                lambda *refs: slice_kernel(total, *refs),
                out_shape=shape((2 * low, count), jnp.int32),
                in_specs=[vmem],
                out_specs=vmem,
                compiler_params=SMALL_PARAMS,
                name="slice",
            )(msg)
            for msg in lists
        ]
        pair, embed = pl.pallas_call(
            lambda *refs: pairs_kernel(n_atoms, *refs),
            out_shape=[shape((total, total), F32), shape((width, total), F32)],
            in_specs=[vmem] * (2 * n_atoms + 1),
            out_specs=[vmem, vmem],
            scratch_shapes=[pltpu.VMEM((n_atoms, EXTRA, count), F32)],
            compiler_params=PAIRS_PARAMS,
            name="pairs",
        )(*lists, *counted, type_table[0])
        force = pl.pallas_call(
            lambda *refs: frame_kernel(n_section, n_atoms, heads, slots, *refs),
            out_shape=shape((8, total), F32),
            in_specs=[vmem] * (n_atoms + n_section + 2),
            out_specs=vmem,
            scratch_shapes=[pltpu.VMEM((n_section, width + WROWS, 4 * width), BF16)],
            compiler_params=FRAME_PARAMS,
            name="frame",
        )(*lists, *weights, pair, embed)

        def joint(x, r):
            if x == 0 and r == 0:
                return force
            pairs = [
                (m * n_atoms + a, dest(n_member, m, r) * n_atoms + dest(n_atoms, a, x))
                for m in range(n_member)
                for a in range(n_atoms)
            ]
            return lax.ppermute(force, ("member", "atoms"), pairs)

        got = [joint(x, r) for x in range(per_section) for r in range(n_member)]
        atom_dev, max_dev, mean_force = pl.pallas_call(
            lambda *refs: emit_kernel(n_member, n_atoms, count, *refs),
            out_shape=[
                shape((per_section, count), F32),
                shape((per_section,), F32),
                shape((3, per_section, count), F32),
            ],
            in_specs=[vmem] * len(got),
            out_specs=[vmem, smem, vmem],
            scratch_shapes=[pltpu.VMEM((n_member, 8, total), F32)],
            compiler_params=SMALL_PARAMS,
            name="emit",
        )(*got)
        return atom_dev, max_dev, jnp.transpose(mean_force, (1, 0, 2))

    return body


def solution(mesh):
    sizes = mesh.shape
    return jax.shard_map(
        shards(sizes["member"], sizes["section"], sizes["atoms"]),
        mesh=mesh,
        in_specs=(
            P(None, None, "atoms"),
            P(None, "atoms"),
            P(None, "atoms", None),
            P(None, "atoms", None),
            P("member", None, None),
            P("member", "section", None),
            P("member", "section", None, None),
            P("member", "section", None, None),
            P("member", "section", None),
        ),
        out_specs=(P("section", "atoms"), P("section"), P("section", None, "atoms")),
        check_vma=False,
    )
```

```python
import math

import jax
import jax.numpy as jnp
from jax import lax
from jax.experimental import pallas as pl
from jax.experimental.pallas import tpu as pltpu
from jax.sharding import PartitionSpec as P

F32 = jnp.float32
BF16 = jnp.bfloat16
EXTRA = 8
NIBBLES = 8
AHEAD = 2
UNROLL = 4
LAG = 2
WROWS = 16
FRAME_PARAMS = pltpu.CompilerParams(vmem_limit_bytes=32 << 20)
PAIRS_PARAMS = pltpu.CompilerParams(vmem_limit_bytes=16 << 20)
SMALL_PARAMS = pltpu.CompilerParams(vmem_limit_bytes=8 << 20)


def dest(axis_size, index, r):
    if axis_size & (axis_size - 1) == 0:
        return index ^ r
    return (index + r) % axis_size


def source(axis_size, index, r):
    if axis_size & (axis_size - 1) == 0:
        return index ^ r
    return (index - r) % axis_size


def exchange(x, axis, axis_size, r):
    if r == 0:
        return x
    return lax.ppermute(x, axis, [(i, dest(axis_size, i, r)) for i in range(axis_size)])


def dot(a, b):
    return lax.dot_general(a, b, (((1,), (0,)), ((), ())), preferred_element_type=F32)


def pack_kernel(n_section, pos_ref, typ_ref, nbr_ref, mask_ref, proj_ref, outw_ref, *refs):
    gain_ref, coef_ref = refs[:2]
    frames = pos_ref.shape[1]
    per_section = frames // n_section
    outs, w_out = refs[2 : 2 + per_section], refs[2 + per_section]
    pos_v, typ_v, nbr_v, mask_v, gain_v, coef_v, sems = refs[3 + per_section :]
    first = lax.axis_index("section") * per_section
    mine = lax.axis_index("atoms") % per_section
    side = outw_ref.shape[0]
    small = [
        pltpu.make_async_copy(pos_ref, pos_v, sems.at[0]),
        pltpu.make_async_copy(typ_ref, typ_v, sems.at[1]),
    ]
    for c in small:
        c.start()
    lists = []
    for x in range(per_section):
        frame = first + dest(per_section, mine, x)
        a = pltpu.make_async_copy(nbr_ref.at[frame], nbr_v.at[x], sems.at[6 + 2 * x])
        b = pltpu.make_async_copy(mask_ref.at[frame], mask_v.at[x], sems.at[7 + 2 * x])
        a.start()
        b.start()
        lists.append((frame, a, b))
    weights = [
        pltpu.make_async_copy(proj_ref, w_out.at[:side, : 3 * side], sems.at[2]),
        pltpu.make_async_copy(outw_ref, w_out.at[:side, 3 * side :], sems.at[3]),
        pltpu.make_async_copy(gain_ref, gain_v, sems.at[4]),
        pltpu.make_async_copy(coef_ref, coef_v, sems.at[5]),
    ]
    for c in weights:
        c.start()
    for c in small:
        c.wait()
    for x, (frame, a, b) in enumerate(lists):
        a.wait()
        b.wait()
        slots = nbr_v.shape[2]
        count = nbr_v.shape[1]
        eff = jnp.where(mask_v[x] != 0, nbr_v[x], -1).astype(F32)
        outs[x][:slots, :] = jnp.transpose(eff)
        rows = [pos_v[c, pl.ds(frame, 1), :] for c in range(3)]
        rows.append(typ_v[pl.ds(frame, 1), :].astype(F32))
        rows.append(jnp.zeros((EXTRA - 4, count), F32))
        outs[x][slots:, :] = jnp.concatenate(rows, axis=0)
    for c in weights:
        c.wait()
    heads = coef_v.shape[1]
    row = jnp.concatenate(
        [gain_v[...], coef_v[...], jnp.zeros((1, 3 * side - heads), BF16)], axis=1
    )
    w_out[side:, :] = jnp.broadcast_to(row.astype(F32), (WROWS, 4 * side)).astype(BF16)


def count_slots(list_ref, slots, total, cnt_ref):
    count = list_ref.shape[1]
    low = total // NIBBLES
    iota = lax.broadcasted_iota(jnp.int32, (low, count), 0)
    cnt_ref[...] = jnp.zeros_like(cnt_ref)
    unroll = math.gcd(slots // 8, UNROLL)

    def chunk(c, carry):
        for u in range(unroll):
            eff = list_ref[pl.ds(c * 8 * unroll + 8 * u, 8), :]
            hi = jnp.floor((eff + 0.5) * (1.0 / low))
            lo = jnp.where(eff < 0, -1.0, eff - hi * low).astype(jnp.int32)
            weight = jnp.left_shift(1, 4 * jnp.maximum(hi, 0.0).astype(jnp.int32))
            nib = None
            for s in range(8):
                one = jnp.where(iota == lo[s : s + 1, :], weight[s : s + 1, :], 0)
                nib = one if nib is None else nib + one
            cnt_ref[:low, :] += nib & 0x0F0F0F0F
            cnt_ref[low:, :] += lax.shift_right_logical(nib, 4) & 0x0F0F0F0F
        return carry

    lax.fori_loop(0, slots // (8 * unroll), chunk, 0)


def slice_kernel(total, msg_ref, cnt_ref):
    count_slots(msg_ref, msg_ref.shape[0] - EXTRA, total, cnt_ref)


def pairs_kernel(n_atoms, *refs):
    msgs, cnt_v = refs[:n_atoms], refs[n_atoms : 2 * n_atoms]
    table_ref, p_ref, h_ref, ext_v = refs[2 * n_atoms :]
    slots = msgs[0].shape[0] - EXTRA
    count = msgs[0].shape[1]
    total = n_atoms * count
    low = total // NIBBLES
    a_idx = lax.axis_index("atoms")
    ext = [msgs[r][slots:, :] for r in range(n_atoms)]
    types = jnp.concatenate(ext, axis=1)[3:4].astype(jnp.int32)
    iota_t = lax.broadcasted_iota(jnp.int32, (table_ref.shape[0], total), 0)
    onehot = (iota_t == types).astype(BF16)
    h_ref[...] = dot(jnp.transpose(table_ref[...]), onehot)
    for r in range(n_atoms):
        ext_v[source(n_atoms, a_idx, r)] = ext[r]
    pos_col = jnp.concatenate([jnp.transpose(ext_v[b]) for b in range(n_atoms)], axis=0)
    for n in range(NIBBLES):
        part = pos_col[n * low : (n + 1) * low]
        cols = [jnp.broadcast_to(part[:, c : c + 1], (low, count)) for c in range(3)]
        for r in range(n_atoms):
            acc = cnt_v[r][low:, :] if n % 2 else cnt_v[r][:low, :]
            hits = (lax.shift_right_logical(acc, 8 * (n // 2)) & 0xFF).astype(F32)
            dist = None
            for c in range(3):
                delta = cols[c] - ext[r][c : c + 1, :]
                dist = delta * delta if dist is None else dist + delta * delta
            p_ref[n * low : (n + 1) * low, r * count : (r + 1) * count] = hits / (
                2.0 + 0.25 * dist
            )


def frame_kernel(n_section, n_atoms, heads, slots, *refs):
    msgs, refs = refs[:n_atoms], refs[n_atoms:]
    weights_in, refs = refs[:n_section], refs[n_section:]
    p_v, embed_ref, out_ref, w_v = refs
    count = msgs[0].shape[1]
    total = n_atoms * count
    width = embed_ref.shape[0]
    head_dim = width // heads
    a_idx = lax.axis_index("atoms")
    s_idx = lax.axis_index("section")
    tile = 256 if total % 256 == 0 else count
    tiles = total // tile
    per_tile = tile // count
    group = max(1, 256 // tile)
    span = [slice(t * tile, (t + 1) * tile) for t in range(tiles)]
    for r in range(n_section):
        w_v[source(n_section, s_idx, r)] = weights_in[r][...]
    pos = jnp.concatenate([msgs[r][slots:, :] for r in range(n_atoms)], axis=1)[:3]
    pos_hi = pos.astype(BF16).astype(F32)
    tail = jnp.concatenate(
        [pos_hi, pos - pos_hi, jnp.ones((1, total), F32), jnp.zeros((9, total), F32)], axis=0
    ).astype(BF16)

    scale = 0.5 / math.sqrt(head_dim)
    h = [embed_ref[:, span[t]] for t in range(tiles)]
    params = {}

    def load(b):
        w = w_v[b]
        row = w[width:]
        gain = jnp.transpose(jnp.broadcast_to(row[:1, :width].astype(F32), (width, width)))
        coef = row[:1, width : width + heads].astype(F32)
        params[b] = jnp.transpose(w[:width]), gain, coef

    state = {}
    force = [None] * tiles
    results = {}
    zeros = {}

    def zero_rows(n):
        if n not in zeros:
            zeros[n] = jnp.zeros((n, tile), BF16)
        return zeros[n]

    def project(b, t):
        if b not in params:
            load(b)
        w, gain, _ = params[b]
        norm = lax.rsqrt(jnp.mean(h[t] * h[t], axis=0, keepdims=True) + 1e-06)
        x = (h[t] * norm * gain[:, :1]).astype(BF16)
        k = jnp.transpose(dot(w[width : 2 * width], x).astype(BF16))
        q = dot(w[:width], x).astype(BF16).astype(F32) * scale
        q_hi = q.astype(BF16)
        q_lo = (q - q_hi.astype(F32)).astype(BF16)
        v = None
        if b + 1 < n_section:
            v = dot(w[2 * width : 3 * width], x).astype(BF16)
        rhs = []
        for first in range(0, heads, group):
            cols = []
            for hd in range(first, first + group):
                rows = []
                for term in (q_hi, q_lo):
                    if hd > 0:
                        rows.append(zero_rows(hd * head_dim))
                    rows.append(term[hd * head_dim : (hd + 1) * head_dim])
                    if hd < heads - 1:
                        rows.append(zero_rows((heads - 1 - hd) * head_dim))
                cols.append(jnp.concatenate(rows, axis=0))
            rhs.append(jnp.concatenate(cols, axis=1))
        k = jnp.concatenate([k, k], axis=1)
        state[b, t] = rhs, k, v

    def score(b, t, jt, g):
        return dot(state[b, jt][1], state[b, t][0][g])

    def consume(unit, value):
        _, t, jt, _ = unit
        p = jnp.concatenate(
            [
                p_v[pl.ds(source(n_atoms, a_idx, r) * count, count), span[t]]
                for r in range(jt * per_tile, (jt + 1) * per_tile)
            ],
            axis=0,
        )
        parts = []
        for i in range(group):
            parts.append(p * jnp.tanh(value[:, i * tile : (i + 1) * tile]) + p)
        return jnp.concatenate(parts, axis=1).astype(BF16)

    def message(unit, value):
        b, t, jt, g = unit
        lhs, base = tail[:, span[jt]], 0
        if b + 1 < n_section:
            base = group * head_dim
            rows = slice(g * base, (g + 1) * base)
            lhs = jnp.concatenate([state[b, jt][2][rows], lhs], axis=0)
        res = dot(lhs, value)
        for i in range(group):
            lanes = slice(i * tile, (i + 1) * tile)
            own = (
                res[base : base + 8, lanes],
                *([res[i * head_dim : (i + 1) * head_dim, lanes]] if base else []),
            )
            key = b, t, g * group + i
            if key in results:
                own = tuple(x + y for x, y in zip(results[key], own))
            results[key] = own

    def finish(b, t):
        w, _, coef = params[b]
        parts = [results.pop((b, t, hd)) for hd in range(heads)]
        if b + 1 < n_section:
            msg = jnp.concatenate([part[1] for part in parts], axis=0) * (1.0 / slots)
            step = dot(w[3 * width :], msg.astype(BF16))
            h[t] = (h[t] + step).astype(BF16).astype(F32)
            project(b + 1, t)
        for hd, part in enumerate(parts):
            term = coef[:, hd : hd + 1] * part[0]
            force[t] = term if force[t] is None else force[t] + term

    last = tiles - 1
    order = [(t, jt) for t in range(last) for jt in range(last)]
    order += [(t, last) for t in range(last)]
    order += [(last, jt) for jt in range(tiles)]
    units = [
        (b, t, jt, g) for b in range(n_section) for t, jt in order for g in range(heads // group)
    ]
    left = {(b, t): tiles * (heads // group) for b in range(n_section) for t in range(tiles)}
    pending, gated = [], []

    def retire():
        if pending:
            gate()
        if len(gated) > LAG or not pending:
            settle()

    def settle():
        unit, value = gated.pop(0)
        b, t = unit[:2]
        message(unit, value)
        left[b, t] -= 1
        if left[b, t] == 0:
            finish(b, t)

    def gate():
        unit, value = pending.pop(0)
        gated.append((unit, consume(unit, value)))

    for t in range(tiles):
        project(0, t)
    for unit in units:
        b, t, jt, _ = unit
        while (b, t) not in state or (b, jt) not in state:
            retire()
        pending.append((unit, score(*unit)))
        while len(pending) > AHEAD:
            retire()
    while pending or gated:
        retire()

    f = jnp.concatenate(force, axis=1)
    out = (f[0:3] + f[3:6] - pos * f[6:7]) * (1.0 / slots)
    out_ref[...] = jnp.concatenate([out, jnp.zeros((5, total), F32)], axis=0)


def emit_kernel(n_member, n_atoms, count, *refs):
    ins, (dev_ref, max_ref, mean_ref, members_v) = refs[:-4], refs[-4:]
    per_section = len(ins) // n_member
    mine = lax.axis_index("atoms") % per_section
    own = lax.axis_index("member")
    for x in range(per_section):
        for r in range(n_member):
            members_v[source(n_member, own, r)] = ins[x * n_member + r][...]
        forces = [members_v[m][:3] for m in range(n_member)]
        mean = sum(forces) * (1.0 / n_member)
        spread = sum(jnp.sum((f - mean) * (f - mean), 0, keepdims=True) for f in forces)
        dev = jnp.sqrt(spread * (1.0 / n_member))
        r = x if n_atoms & (n_atoms - 1) == 0 else (-x) % n_atoms
        lanes = slice(r * count, (r + 1) * count)
        frame = source(per_section, mine, x)
        dev_ref[pl.ds(frame, 1), :] = dev[:, lanes]
        for c in range(3):
            mean_ref[c, pl.ds(frame, 1), :] = mean[c : c + 1, lanes]
        max_ref[frame] = jnp.max(dev)


def shards(n_member, n_section, n_atoms):
    def body(
        positions,
        atom_types,
        neighbors,
        nbr_mask,
        type_table,
        norm_gain,
        proj_weight,
        out_weight,
        force_coef,
    ):
        frames = positions.shape[0]
        per_section = frames // n_section
        count, slots = neighbors.shape[1:]
        total = count * n_atoms
        heads = force_coef.shape[-1]
        width = out_weight.shape[-1]
        any_spec = pl.BlockSpec(memory_space=pl.ANY)
        vmem = pl.BlockSpec(memory_space=pltpu.VMEM)
        smem = pl.BlockSpec(memory_space=pltpu.SMEM)
        shape = jax.ShapeDtypeStruct

        *packed, own_w = pl.pallas_call(
            lambda *refs: pack_kernel(n_section, *refs),
            out_shape=[shape((slots + EXTRA, count), F32)] * per_section
            + [shape((width + WROWS, 4 * width), BF16)],
            in_specs=[any_spec] * 8,
            out_specs=[vmem] * (per_section + 1),
            scratch_shapes=[
                pltpu.VMEM((3, frames, count), F32),
                pltpu.VMEM((frames, count), jnp.int32),
                pltpu.VMEM((per_section, count, slots), jnp.int32),
                pltpu.VMEM((per_section, count, slots), jnp.int32),
                pltpu.VMEM((1, width), BF16),
                pltpu.VMEM((1, heads), BF16),
                pltpu.SemaphoreType.DMA((6 + 2 * per_section,)),
            ],
            compiler_params=SMALL_PARAMS,
            name="pack",
        )(
            *[
                pltpu.with_memory_space_constraint(x, pltpu.HBM)
                for x in (
                    jnp.transpose(positions, (1, 0, 2)),
                    atom_types,
                    neighbors,
                    nbr_mask,
                    proj_weight[0, 0],
                    out_weight[0, 0],
                    norm_gain[0],
                    force_coef[0],
                )
            ]
        )
        lists = [exchange(packed[r % per_section], "atoms", n_atoms, r) for r in range(n_atoms)]
        weights = [exchange(own_w, "section", n_section, r) for r in range(n_section)]

        low = total // NIBBLES
        counted = [
            pl.pallas_call(
                lambda *refs: slice_kernel(total, *refs),
                out_shape=shape((2 * low, count), jnp.int32),
                in_specs=[vmem],
                out_specs=vmem,
                compiler_params=SMALL_PARAMS,
                name="slice",
            )(msg)
            for msg in lists
        ]
        pair, embed = pl.pallas_call(
            lambda *refs: pairs_kernel(n_atoms, *refs),
            out_shape=[shape((total, total), F32), shape((width, total), F32)],
            in_specs=[vmem] * (2 * n_atoms + 1),
            out_specs=[vmem, vmem],
            scratch_shapes=[pltpu.VMEM((n_atoms, EXTRA, count), F32)],
            compiler_params=PAIRS_PARAMS,
            name="pairs",
        )(*lists, *counted, type_table[0])
        force = pl.pallas_call(
            lambda *refs: frame_kernel(n_section, n_atoms, heads, slots, *refs),
            out_shape=shape((8, total), F32),
            in_specs=[vmem] * (n_atoms + n_section + 2),
            out_specs=vmem,
            scratch_shapes=[pltpu.VMEM((n_section, width + WROWS, 4 * width), BF16)],
            compiler_params=FRAME_PARAMS,
            name="frame",
        )(*lists, *weights, pair, embed)

        def joint(x, r):
            if x == 0 and r == 0:
                return force
            pairs = [
                (m * n_atoms + a, dest(n_member, m, r) * n_atoms + dest(n_atoms, a, x))
                for m in range(n_member)
                for a in range(n_atoms)
            ]
            return lax.ppermute(force, ("member", "atoms"), pairs)

        got = [joint(x, r) for x in range(per_section) for r in range(n_member)]
        atom_dev, max_dev, mean_force = pl.pallas_call(
            lambda *refs: emit_kernel(n_member, n_atoms, count, *refs),
            out_shape=[
                shape((per_section, count), F32),
                shape((per_section,), F32),
                shape((3, per_section, count), F32),
            ],
            in_specs=[vmem] * len(got),
            out_specs=[vmem, smem, vmem],
            scratch_shapes=[pltpu.VMEM((n_member, 8, total), F32)],
            compiler_params=SMALL_PARAMS,
            name="emit",
        )(*got)
        return atom_dev, max_dev, jnp.transpose(mean_force, (1, 0, 2))

    return body


def solution(mesh):
    sizes = mesh.shape
    return jax.shard_map(
        shards(sizes["member"], sizes["section"], sizes["atoms"]),
        mesh=mesh,
        in_specs=(
            P(None, None, "atoms"),
            P(None, "atoms"),
            P(None, "atoms", None),
            P(None, "atoms", None),
            P("member", None, None),
            P("member", "section", None),
            P("member", "section", None, None),
            P("member", "section", None, None),
            P("member", "section", None),
        ),
        out_specs=(P("section", "atoms"), P("section"), P("section", None, "atoms")),
        check_vma=False,
    )
```
